512 devices in a mesh: seq: 64 (over z, y), head: 8 (over x, core).
Axes of the slice: x: 4, y: 4, z: 16, core: 2. Of those that a mesh axis runs over, the one named last changes fastest.
Arguments:
- queries: bfloat16 [24576, 4096], P('seq', 'head'), may hold values from -32 to 32
- keys: bfloat16 [24576, 1024], P('seq', 'head'), may hold values from -9 to 9
- values: bfloat16 [24576, 1024], P('seq', 'head'), may hold values from -96 to 96
- block_ids: int32 [64, 32, 3], P('seq', 'head'), may hold values from 0 to 63, as said below
- out_weight: bfloat16 [4096, 4096], P('head'), may hold values from -0.09375 to 0.09375
Outputs:
- projected: bfloat16 [4096, 24576], P('head', 'seq')
The draws below stay inside these ranges and needn't reach their ends.
Inputs may be any that keep to these rules, and one draw needn't show every extreme that they name: `block_ids`: for each query block and key/value head, the 12 ids of the query heads that share that key/value head are all different. An id at or above its own query block's index names a block that the causal rule removes.
All inputs are finite; a program needn't handle non-finite values.
Results may differ from the reference program's by a relative error of at most 0.02.
Values may be sent and summed in bfloat16 or wider, within the bound.
No kernel may reach another device: no remote copies, remote signals or barrier semaphores. Data moves between devices by JAX's collectives and lax.ppermute only.
A program may use at most 128 MiB of HBM per device.

```python
import math
import jax
import jax.numpy as jnp
from jax import lax

D = 4096
QUERY_HEADS = 32
KEY_VALUE_HEADS = 8
HEAD_DIMENSION = 128
BLOCK_TOKENS = 384
TOPK = 3
QUERY_PER_KEY = 4
BLOCK_COUNT = 64
SEQUENCE_TOKENS = 24576
N_HEAD = 8


def sampled_keys(key):
    random_seed_key = jax.random.fold_in(key, 11)
    raw_logits = jnp.clip(jax.random.normal(random_seed_key, (SEQUENCE_TOKENS, KEY_VALUE_HEADS * HEAD_DIMENSION), jnp.float32), -4.0, 4.0)
    return raw_logits


def draw_keys(key, part):
    return sampled_keys(key).astype(jnp.bfloat16)


def draw_queries(key, part):
    random_seed_key = jax.random.fold_in(key, 21)
    raw_logits = jnp.clip(jax.random.normal(random_seed_key, (SEQUENCE_TOKENS, QUERY_HEADS * HEAD_DIMENSION), jnp.float32), -4.0, 4.0)
    return raw_logits.astype(jnp.bfloat16)


def draw_block_ids(key, part):
    picked_block_index = QUERY_PER_KEY * TOPK
    block_scores = jax.random.randint(jax.random.fold_in(key, 31), (BLOCK_COUNT, KEY_VALUE_HEADS, BLOCK_COUNT), 0, 1024)
    hot = jax.random.randint(jax.random.fold_in(key, 32), (BLOCK_COUNT,), 0, 8) == 0
    blocks = jnp.arange(BLOCK_COUNT, dtype=jnp.int32)
    earlier = blocks[None, None, :] < blocks[:, None, None]
    ranked = jnp.where(earlier, (block_scores + jnp.where(hot, 1024, 0)[None, None, :]) * BLOCK_COUNT + blocks[None, None, :], -1 - blocks[None, None, :])
    first_pick = (blocks[:, None, None] == BLOCK_COUNT - 1) & (blocks[None, None, :] == 0)
    ranked = jnp.where(first_pick, 4096 * BLOCK_COUNT, ranked)
    unused, picked = lax.top_k(ranked, picked_block_index)
    permute_rows = jax.random.randint(jax.random.fold_in(key, 33), (BLOCK_COUNT, KEY_VALUE_HEADS, picked_block_index), 0, 4096) * picked_block_index + jnp.arange(picked_block_index, dtype=jnp.int32)
    order = jnp.argsort(permute_rows, axis=-1)
    picked = jnp.take_along_axis(picked, order, axis=-1)
    return picked.reshape(BLOCK_COUNT, QUERY_HEADS, TOPK).astype(jnp.int32)


def level_of(key, extent, split, least, top_value):
    def one(axis_at, shards_of):
        draws = jax.random.uniform(jax.random.fold_in(jax.random.fold_in(key, 6), axis_at), (shards_of,), jnp.float32, least / len(split), top_value / len(split))
        return jnp.repeat(jnp.exp(draws), extent[axis_at] // shards_of).reshape((-1,) + (1,) * (len(extent) - axis_at - 1))

    gain = one(*split[0])
    for cut in split[1:]:
        gain = gain * one(*cut)
    return gain


def scatter_about(rng, dims, deviation, bound, cuts=(), kind=jnp.bfloat16):
    drawn = jax.random.normal(rng, dims, jnp.float32) * deviation
    if len(cuts) > 0:
        drawn = level_of(rng, dims, cuts, -0.22, 0.18) * drawn
    return jnp.clip(drawn, min=-bound, max=bound).astype(kind)


def setup_inputs(seed: int = 0) -> dict:
    key_list = jax.random.split(jax.random.key(seed), 6)
    return {
        "queries": draw_queries(jax.random.fold_in(key_list[5], 71), 0),
        "keys": draw_keys(jax.random.fold_in(key_list[5], 71), 0),
        "values": scatter_about(key_list[2], (SEQUENCE_TOKENS, KEY_VALUE_HEADS * HEAD_DIMENSION), 16.0, 96.0, ((0, 64), (1, 8))),
        "block_ids": draw_block_ids(jax.random.fold_in(key_list[5], 71), 0),
        "out_weight": scatter_about(key_list[4], (QUERY_HEADS * HEAD_DIMENSION, D), (QUERY_HEADS * HEAD_DIMENSION) ** -0.5, 0.09375, ((0, 8),)),
    }


def block_part(query_tile, key_tile, value_tile, keep):
    block_scores = jnp.einsum('hqd,hkd->hqk', query_tile.astype(jnp.float32), key_tile.astype(jnp.float32)) * (1.0 / math.sqrt(HEAD_DIMENSION))
    if keep is not None:
        block_scores = jnp.where(keep, block_scores, -1e+30)
    top = lax.optimization_barrier(jnp.max(block_scores, axis=-1))
    prob = jnp.exp(block_scores - top[..., None])
    if keep is not None:
        prob = jnp.where(keep, prob, 0.0)
    total = lax.optimization_barrier(jnp.sum(prob, axis=-1))
    rounded = lax.optimization_barrier(prob.astype(jnp.bfloat16))
    part = jnp.einsum('hqk,hkd->hqd', rounded.astype(jnp.float32), value_tile.astype(jnp.float32)).astype(jnp.bfloat16)
    return (part, top, total)

def reference(queries, keys, values, block_ids, out_weight):
    q_blocks = queries.reshape(BLOCK_COUNT, BLOCK_TOKENS, QUERY_HEADS, HEAD_DIMENSION)
    key_block_tiles = keys.reshape(BLOCK_COUNT, BLOCK_TOKENS, KEY_VALUE_HEADS, HEAD_DIMENSION).transpose(0, 2, 1, 3)
    value_block_tiles = values.reshape(BLOCK_COUNT, BLOCK_TOKENS, KEY_VALUE_HEADS, HEAD_DIMENSION).transpose(0, 2, 1, 3)
    head_kv = jnp.arange(QUERY_HEADS, dtype=jnp.int32) // QUERY_PER_KEY
    position = jnp.arange(BLOCK_TOKENS, dtype=jnp.int32)
    causal = position[:, None] >= position[None, :]
    weight_groups = out_weight.reshape(N_HEAD, QUERY_HEADS * HEAD_DIMENSION // N_HEAD, D).astype(jnp.float32)

    def one_block(index):
        query_rows = q_blocks[index].transpose(1, 0, 2)
        own_part, own_top, own_total = block_part(query_rows, key_block_tiles[index][head_kv], value_block_tiles[index][head_kv], causal[None])
        chosen = block_ids[index]
        live = chosen < index
        k_sel = key_block_tiles[chosen, head_kv[:, None]].reshape(QUERY_HEADS * TOPK, BLOCK_TOKENS, HEAD_DIMENSION)
        v_sel = value_block_tiles[chosen, head_kv[:, None]].reshape(QUERY_HEADS * TOPK, BLOCK_TOKENS, HEAD_DIMENSION)
        repeated = jnp.repeat(query_rows, TOPK, axis=0)
        sel_part, sel_top, sel_total = block_part(repeated, k_sel, v_sel, None)
        sel_part = sel_part.reshape(QUERY_HEADS, TOPK, BLOCK_TOKENS, HEAD_DIMENSION)
        sel_top = sel_top.reshape(QUERY_HEADS, TOPK, BLOCK_TOKENS)
        sel_total = sel_total.reshape(QUERY_HEADS, TOPK, BLOCK_TOKENS)
        safe_top = jnp.where(live[..., None], sel_top, own_top[:, None, :])
        top = jnp.maximum(own_top, lax.optimization_barrier(jnp.max(safe_top, axis=1)))
        own_weight = jnp.exp(own_top - top)
        sel_weight = jnp.where(live[..., None], jnp.exp(safe_top - top[:, None, :]), 0.0)
        total = own_weight * own_total + lax.optimization_barrier(jnp.sum(sel_weight * sel_total, axis=1))
        accum = own_weight[..., None] * own_part.astype(jnp.float32) + lax.optimization_barrier(jnp.sum(sel_weight[..., None] * sel_part.astype(jnp.float32), axis=1))
        attended = (accum / total[..., None]).transpose(1, 0, 2).reshape(BLOCK_TOKENS, QUERY_HEADS * HEAD_DIMENSION).astype(jnp.bfloat16)
        grouped = attended.reshape(BLOCK_TOKENS, N_HEAD, QUERY_HEADS * HEAD_DIMENSION // N_HEAD).astype(jnp.float32)
        pieces = jnp.einsum('tnf,nfd->ntd', grouped, weight_groups).astype(jnp.bfloat16)
        pieces = lax.optimization_barrier(pieces)
        return lax.optimization_barrier(jnp.sum(pieces.astype(jnp.float32), axis=0)).astype(jnp.bfloat16)
    mixed = lax.map(one_block, jnp.arange(BLOCK_COUNT, dtype=jnp.int32))
    return mixed.reshape(SEQUENCE_TOKENS, D).T
```

```python
import math

import jax
import jax.numpy as jnp
from jax import lax
from jax.experimental import pallas as pl
from jax.experimental.pallas import tpu as pltpu
from jax.sharding import Mesh, PartitionSpec as P

HD = 128
HEADS = 4
TOP = 3
NZ, NY, NX = 16, 4, 4
TOK = 384
SL = TOK // NY
EXT = HEADS * HD + 16
LOG2E = 1.4426950408889634
COEF = LOG2E / math.sqrt(HD)
DEAD = -1e30
SLOTS = (2, 10, 14, 7, 3, 11, 15, 4, 0, 8, 12, 5, 1, 9, 13, 6)


def shift(n, s):
    return [(i, (i + s) % n) for i in range(n)]


def tn(a, b):
    return lax.dot_general(a, b, (((0,), (0,)), ((), ())), preferred_element_type=jnp.float32)


def own_kernel(q_ref, k_ref, v_ref, o_ref, lse_ref):
    keep = lax.broadcasted_iota(jnp.int32, (TOK, TOK), 0) <= lax.broadcasted_iota(
        jnp.int32, (TOK, TOK), 1
    )
    k = k_ref[...]
    v = v_ref[...]
    rows = []
    for h in range(HEADS):
        s = jnp.dot(k, q_ref[h * HD : (h + 1) * HD, :], preferred_element_type=jnp.float32)
        s = jnp.where(keep, s * COEF, DEAD)
        top = jnp.max(s, axis=0, keepdims=True)
        p = jnp.exp2(s - top)
        total = jnp.sum(p, axis=0, keepdims=True)
        o = tn(v, p.astype(jnp.bfloat16)) * (1.0 / total)
        o_ref[h * HD : (h + 1) * HD, :] = o.astype(jnp.bfloat16)
        rows.append(top + jnp.log2(total))
    lse_ref[...] = jnp.concatenate(rows + rows, axis=0)


def slices_of(idx_ref, bias_ref, kv, q_ref, o_ref, base):
    rows = []
    for h in range(HEADS):
        at = base + h * TOP
        picked = [kv[idx_ref[at + j]] for j in range(TOP)]
        k = jnp.concatenate([t[:, :HD] for t in picked], axis=0)
        v = jnp.concatenate([t[:, HD:] for t in picked], axis=0)
        s = jnp.dot(k, q_ref[h * HD : (h + 1) * HD, :], preferred_element_type=jnp.float32)
        s = [s[j * SL : (j + 1) * SL] * COEF + bias_ref[at + j] for j in range(TOP)]
        s = jnp.concatenate(s, axis=0)
        top = jnp.max(s, axis=0, keepdims=True)
        p = jnp.exp2(s - top)
        total = jnp.sum(p, axis=0, keepdims=True)
        o = tn(v, p.astype(jnp.bfloat16)) * (1.0 / total)
        o_ref[h * HD : (h + 1) * HD, :] = o.astype(jnp.bfloat16)
        lse = top + jnp.log2(total)
        hi = lse.astype(jnp.bfloat16).astype(jnp.float32)
        mid = (lse - hi).astype(jnp.bfloat16).astype(jnp.float32)
        rows += [hi, mid, lse - hi - mid]
    rows += [jnp.zeros((4, TOK), jnp.float32)]
    o_ref[HEADS * HD :, :] = jnp.concatenate(rows, axis=0).astype(jnp.bfloat16)


def make_slices(n):
    def kernel(idx_ref, bias_ref, a0, a1, a2, a3, a4, *rest):
        q_refs, o_refs, (kv, sems) = rest[:n], rest[n : 2 * n], rest[2 * n :]
        copies = []
        at = 0
        for i, src in enumerate((a0, a1, a2, a3, a4)):
            width = src.shape[0]
            copies.append(pltpu.make_async_copy(src, kv.at[pl.ds(at, width)], sems.at[i]))
            at += width
        for c in copies:
            c.start()
        for c in copies:
            c.wait()
        for i in range(n):
            slices_of(idx_ref, bias_ref, kv, q_refs[i], o_refs[i], i * HEADS * TOP)

    smem = pl.BlockSpec(memory_space=pltpu.SMEM)
    vmem = pl.BlockSpec(memory_space=pltpu.VMEM)
    hbm = pl.BlockSpec(memory_space=pl.ANY)
    return pl.pallas_call(
        kernel,
        in_specs=[smem, smem] + [hbm] * 5 + [vmem] * n,
        out_specs=[vmem] * n,
        out_shape=[jax.ShapeDtypeStruct((EXT, TOK), jnp.bfloat16)] * n,
        scratch_shapes=[
            pltpu.VMEM((NZ * NY, SL, 2 * HD), jnp.bfloat16),
            pltpu.SemaphoreType.DMA((5,)),
        ],
    )


def merge_kernel(own_ref, lse_ref, p0, p1, p2, p3, out_ref):
    parts = (p0, p1, p2, p3)
    tails = [p[HEADS * HD :, :].astype(jnp.float32) for p in parts]
    for h in range(HEADS):
        span = slice(h * HD, (h + 1) * HD)
        own = lse_ref[h : h + 1, :]
        lses = [
            t[3 * h : 3 * h + 1] + t[3 * h + 1 : 3 * h + 2] + t[3 * h + 2 : 3 * h + 3]
            for t in tails
        ]
        top = own
        for x in lses:
            top = jnp.maximum(top, x)
        w = jnp.exp2(own - top)
        total = w
        acc = w * own_ref[span, :].astype(jnp.float32)
        for p, x in zip(parts, lses):
            w = jnp.exp2(x - top)
            total = total + w
            acc = acc + w * p[span, :].astype(jnp.float32)
        out_ref[span, :] = (acc * (1.0 / total)).astype(jnp.bfloat16)


def local(queries, keys, values, block_ids, out_weight):
    z = lax.axis_index("z")
    y = lax.axis_index("y")
    x = lax.axis_index("x")
    core = lax.axis_index("core")
    kv = jnp.concatenate([keys, values], axis=1).reshape(NY, SL, 2 * HD)
    row = lax.all_to_all(kv, "y", 0, 0)
    far = lax.ppermute(row, "z", shift(NZ, 8))
    up = lax.ppermute(row, "z", shift(NZ, 4))
    down = lax.ppermute(row, "z", shift(NZ, -4))
    c = jnp.concatenate([far, up, row, down], axis=0)
    n1 = lax.ppermute(c, "z", shift(NZ, 1))
    n2 = lax.ppermute(c, "z", shift(NZ, -1))
    m1 = lax.ppermute(c[NY : 3 * NY], "z", shift(NZ, 2))
    m2 = lax.ppermute(c[2 * NY :], "z", shift(NZ, -2))
    qt = queries.T
    id_rows = jnp.zeros((16, TOK), jnp.bfloat16)
    id_rows = lax.dynamic_update_slice(
        id_rows, block_ids.reshape(1, HEADS * TOP).astype(jnp.bfloat16), (0, 0)
    )
    qx = jnp.concatenate([qt, id_rows], axis=0)
    qs = [qx] + [lax.ppermute(qx, "y", shift(NY, s)) for s in (1, 2, 3)]
    ids = jnp.stack(
        [a[HEADS * HD, : HEADS * TOP].astype(jnp.int32) for a in qs], axis=0
    )
    theirs = z * NY + (y - jnp.arange(NY, dtype=jnp.int32)) % NY
    bias = jnp.where(ids < theirs[:, None], 0.0, DEAD).astype(jnp.float32)
    slot = jnp.array(SLOTS, jnp.int32)[(ids // NY - z) % NZ] * NY + ids % NY
    vmem = pl.BlockSpec(memory_space=pltpu.VMEM)
    own, own_lse = pl.pallas_call(
        own_kernel,
        in_specs=[vmem] * 3,
        out_specs=[vmem] * 2,
        out_shape=[
            jax.ShapeDtypeStruct((HEADS * HD, TOK), jnp.bfloat16),
            jax.ShapeDtypeStruct((2 * HEADS, TOK), jnp.float32),
        ],
    )(qt, keys, values)
    gathered = (c, n1, n2, m1, m2)
    q2, q1, q3 = qs[2], qs[1], qs[3]
    order = jnp.array([2, 1, 3], jnp.int32)
    o2, o1, o3 = make_slices(3)(
        slot[order].reshape(-1), bias[order].reshape(-1), *gathered, q2, q1, q3
    )
    r2 = lax.ppermute(o2, "y", shift(NY, -2))
    r1 = lax.ppermute(o1, "y", shift(NY, -1))
    r3 = lax.ppermute(o3, "y", shift(NY, -3))
    (o0,) = make_slices(1)(slot[0], bias[0], *gathered, qs[0])
    att = pl.pallas_call(
        merge_kernel,
        in_specs=[vmem] * 6,
        out_specs=vmem,
        out_shape=jax.ShapeDtypeStruct((HEADS * HD, TOK), jnp.bfloat16),
    )(own, own_lse, o0, r1, r2, r3)
    pair = [(0, 1), (1, 0)]
    feats = out_weight.reshape(HEADS * HD, NX, 2, HEADS * HD)
    w_mine = lax.dynamic_index_in_dim(feats, core, axis=2, keepdims=False)
    w_give = lax.dynamic_index_in_dim(feats, 1 - core, axis=2, keepdims=False)
    w_got = lax.ppermute(w_give, "core", pair)
    w = jnp.concatenate([w_mine, w_got], axis=0)
    att_got = lax.ppermute(att, "core", pair)
    att_both = jnp.concatenate([att, att_got], axis=0)

    def piece(s):
        cut = lax.dynamic_index_in_dim(w, (x + s) % NX, axis=1, keepdims=False)
        return tn(cut, att_both)

    got = [
        lax.ppermute(piece(s).astype(jnp.bfloat16), "x", shift(NX, s)) for s in (2, 1, 3)
    ]
    total = piece(0)
    for g in got:
        total = total + g.astype(jnp.float32)
    return total.astype(jnp.bfloat16)


def solution(mesh):
    grid = Mesh(mesh.devices.reshape(NZ, NY, NX, 2), ("z", "y", "x", "core"))
    rows, cols = ("z", "y"), ("x", "core")
    return jax.shard_map(
        local,
        mesh=grid,
        in_specs=(P(rows, cols), P(rows, cols), P(rows, cols), P(rows, cols, None), P(cols, None)),
        out_specs=P(cols, rows),
        check_vma=False,
    )
```

```python
import math

import jax
import jax.numpy as jnp
from jax import lax
from jax.experimental import pallas as pl
from jax.experimental.pallas import tpu as pltpu
from jax.sharding import Mesh, PartitionSpec as P


HD = 128
HEADS = 4
HALF = HEADS * HD
TOP = 3
NZ, NY, NX = 16, 4, 4
TOK = 384
SL = TOK // NY
EXT = HALF + 16
LOG2E = 1.4426950408889634
COEF = LOG2E / math.sqrt(HD)
DEAD = -1e30
NONE = NZ * NY
SLOTS = (2, 10, 14, 7, 3, 11, 15, 4, 0, 8, 12, 5, 1, 9, 13, 6)


def pallas(mib, kernel, **kw):
    grant = pltpu.CompilerParams(vmem_limit_bytes=mib * 1024 * 1024)
    return pl.pallas_call(kernel, compiler_params=grant, **kw)


def send(a, axis, s):
    n = lax.axis_size(axis)
    return lax.ppermute(a, axis, [(i, (i + s) % n) for i in range(n)])


def tn(a, b):
    return lax.dot_general(a, b, (((0,), (0,)), ((), ())), preferred_element_type=jnp.float32)


def pack_kernel(k_ref, v_ref, out_ref):
    for y in range(NY):
        out_ref[y, :, :HD] = k_ref[y * SL : (y + 1) * SL, :]
        out_ref[y, :, HD:] = v_ref[y * SL : (y + 1) * SL, :]


def own_kernel(code_ref, q_ref, k_ref, v_ref, qx_ref, o_ref, lse_ref):
    keep = lax.broadcasted_iota(jnp.int32, (TOK, TOK), 0) <= lax.broadcasted_iota(
        jnp.int32, (TOK, TOK), 1
    )
    k = k_ref[...]
    v = v_ref[...]
    rows = []
    for h in range(HEADS):
        q = q_ref[:, h * HD : (h + 1) * HD].T
        qx_ref[h * HD : (h + 1) * HD, :] = q
        s = jnp.dot(k, q, preferred_element_type=jnp.float32)
        s = jnp.where(keep, s * COEF, DEAD)
        top = jnp.max(s, axis=0, keepdims=True)
        p = jnp.exp2(s - top)
        total = jnp.sum(p, axis=0, keepdims=True)
        o = tn(v, p.astype(jnp.bfloat16)) * (1.0 / total)
        o_ref[h * HD : (h + 1) * HD, :] = o.astype(jnp.bfloat16)
        rows.append(top + jnp.log2(total))
    lse_ref[...] = jnp.concatenate(rows + rows, axis=0)
    lane = lax.broadcasted_iota(jnp.int32, (16, TOK), 1)
    codes = jnp.zeros((16, TOK), jnp.float32)
    for i in range(HEADS * TOP):
        codes = jnp.where(lane == i, code_ref[i].astype(jnp.float32), codes)
    qx_ref[HALF:, :] = codes.astype(jnp.bfloat16)


def slices_of(code_ref, kv_ref, q_ref, o_ref, base):
    rows = []
    for h in range(HEADS):
        codes = [code_ref[base + h * TOP + j] for j in range(TOP)]
        picked = [kv_ref[jnp.minimum(c, NONE - 1)] for c in codes]
        bias = [jnp.where(c < NONE, 0.0, DEAD).astype(jnp.float32) for c in codes]
        k = jnp.concatenate([t[:, :HD] for t in picked], axis=0)
        v = jnp.concatenate([t[:, HD:] for t in picked], axis=0)
        s = jnp.dot(k, q_ref[h * HD : (h + 1) * HD, :], preferred_element_type=jnp.float32)
        s = [s[j * SL : (j + 1) * SL] * COEF + bias[j] for j in range(TOP)]
        s = jnp.concatenate(s, axis=0)
        top = jnp.max(s, axis=0, keepdims=True)
        p = jnp.exp2(s - top)
        total = jnp.sum(p, axis=0, keepdims=True)
        o = tn(v, p.astype(jnp.bfloat16)) * (1.0 / total)
        o_ref[h * HD : (h + 1) * HD, :] = o.astype(jnp.bfloat16)
        lse = top + jnp.log2(total)
        hi = lse.astype(jnp.bfloat16).astype(jnp.float32)
        mid = (lse - hi).astype(jnp.bfloat16).astype(jnp.float32)
        rows += [hi, mid, lse - hi - mid]
    rows += [jnp.zeros((4, TOK), jnp.float32)]
    o_ref[HALF:, :] = jnp.concatenate(rows, axis=0).astype(jnp.bfloat16)


def slices_kernel(code_ref, kv_ref, *rest):
    n = len(rest) // 2
    for i in range(n):
        slices_of(code_ref, kv_ref, rest[i], rest[n + i], i * HEADS * TOP)


def merge_kernel(own_ref, lse_ref, p0, p1, p2, p3, out_ref):
    parts = (p0, p1, p2, p3)
    tails = [p[HALF:, :].astype(jnp.float32) for p in parts]
    for h in range(HEADS):
        span = slice(h * HD, (h + 1) * HD)
        own = lse_ref[h : h + 1, :]
        lses = [
            t[3 * h : 3 * h + 1] + t[3 * h + 1 : 3 * h + 2] + t[3 * h + 2 : 3 * h + 3]
            for t in tails
        ]
        top = own
        for x in lses:
            top = jnp.maximum(top, x)
        w = jnp.exp2(own - top)
        total = w
        acc = w * own_ref[span, :].astype(jnp.float32)
        for p, x in zip(parts, lses):
            w = jnp.exp2(x - top)
            total = total + w
            acc = acc + w * p[span, :].astype(jnp.float32)
        out_ref[span, :] = (acc * (1.0 / total)).astype(jnp.bfloat16)


def turn_kernel(cols_ref, mine_ref, got_ref, out_ref):
    out_ref[0, :, :HALF] = mine_ref[...].T
    out_ref[0, :, HALF:] = got_ref[...].T


def piece_of(w_ref, s, mine_ref, got_ref):
    out = jnp.dot(w_ref[s, :, :HALF], mine_ref[...], preferred_element_type=jnp.float32)
    return out + jnp.dot(w_ref[s, :, HALF:], got_ref[...], preferred_element_type=jnp.float32)


def pieces_kernel(w_ref, mine_ref, got_ref, *outs):
    for s, out in zip((2, 1, 3), outs):
        out[...] = piece_of(w_ref, s, mine_ref, got_ref).astype(jnp.bfloat16)


def mine_kernel(w_ref, mine_ref, got_ref, out_ref):
    out_ref[...] = piece_of(w_ref, 0, mine_ref, got_ref)


def sum_kernel(mine_ref, g1, g2, g3, out_ref):
    out = mine_ref[...]
    for g in (g1, g2, g3):
        out += g[...].astype(jnp.float32)
    out_ref[...] = out.astype(jnp.bfloat16)


def bf16(*shape):
    return jax.ShapeDtypeStruct(shape, jnp.bfloat16)


def f32(*shape):
    return jax.ShapeDtypeStruct(shape, jnp.float32)


def steps(queries, keys, values, block_ids, out_weight):
    z = lax.axis_index("z")
    y = lax.axis_index("y")
    x = lax.axis_index("x")
    core = lax.axis_index("core")
    vmem = pl.BlockSpec(memory_space=pltpu.VMEM)
    smem = pl.BlockSpec(memory_space=pltpu.SMEM)
    packed = pallas(
        4, pack_kernel, in_specs=[vmem] * 2, out_specs=vmem, out_shape=bf16(NY, SL, 2 * HD)
    )(keys, values)
    row = lax.all_to_all(packed, "y", 0, 0)
    ids = block_ids.reshape(HEADS * TOP)
    slot = jnp.zeros_like(ids)
    offset = (ids // NY - z) % NZ
    for d, place in enumerate(SLOTS):
        slot = jnp.where(offset == d, place, slot)
    code = jnp.where(ids < z * NY + y, slot * NY + ids % NY, NONE)
    up = send(row, "z", 4)
    down = send(row, "z", -4)
    w_got = send(out_weight, "core", 1)
    qx, own, own_lse = pallas(
        8,
        own_kernel,
        in_specs=[smem] + [vmem] * 3,
        out_specs=[vmem] * 3,
        out_shape=[bf16(EXT, TOK), bf16(HALF, TOK), f32(2 * HEADS, TOK)],
    )(code, queries, keys, values)
    order = (2, 1, 3)
    qs = [send(qx, "y", s) for s in order]
    far1 = send(up[: NY // 2], "z", 4)
    far2 = send(down[NY // 2 :], "z", -4)
    c = jnp.concatenate([far1, far2, up, row, down], axis=0)
    n1 = send(c, "z", 1)
    n2 = send(c, "z", -1)
    codes = jnp.stack([a[HALF, : HEADS * TOP] for a in qs], axis=0).astype(jnp.int32).reshape(-1)
    cols = (x + jnp.arange(NX, dtype=jnp.int32)) % NX * 2 + core
    w = pallas(
        12,
        turn_kernel,
        grid_spec=pltpu.PrefetchScalarGridSpec(
            num_scalar_prefetch=1,
            grid=(NX,),
            in_specs=[pl.BlockSpec((HALF, HALF), lambda s, cols: (0, cols[s]))] * 2,
            out_specs=pl.BlockSpec((1, HALF, 2 * HALF), lambda s, cols: (s, 0, 0)),
        ),
        out_shape=bf16(NX, HALF, 2 * HALF),
    )(cols, out_weight, w_got)
    m1 = send(n1[NY : 3 * NY], "z", 1)
    m2 = send(n2[2 * NY :], "z", -1)
    kv = jnp.concatenate([c, n1, n2, m1, m2], axis=0)
    parts = pallas(
        12,
        slices_kernel,
        in_specs=[smem] + [vmem] * 4,
        out_specs=[vmem] * 3,
        out_shape=[bf16(EXT, TOK)] * 3,
    )(codes, kv, *qs)
    back = [send(o, "y", -s) for s, o in zip(order, parts)]
    (home,) = pallas(
        12,
        slices_kernel,
        in_specs=[smem] + [vmem] * 2,
        out_specs=[vmem],
        out_shape=[bf16(EXT, TOK)],
    )(code, kv, qx)
    att = pallas(
        8, merge_kernel, in_specs=[vmem] * 6, out_specs=vmem, out_shape=bf16(HALF, TOK)
    )(own, own_lse, home, *back)
    att_got = send(att, "core", 1)
    pieces = pallas(
        16,
        pieces_kernel,
        in_specs=[vmem] * 3,
        out_specs=[vmem] * 3,
        out_shape=[bf16(HALF, TOK)] * 3,
    )(w, att, att_got)
    got = [send(p, "x", s) for s, p in zip(order, pieces)]
    mine = pallas(
        12, mine_kernel, in_specs=[vmem] * 3, out_specs=vmem, out_shape=f32(HALF, TOK)
    )(w, att, att_got)
    return pallas(
        8, sum_kernel, in_specs=[vmem] * 4, out_specs=vmem, out_shape=bf16(HALF, TOK)
    )(mine, *got)


def solution(mesh):
    axes = ("z", "y", "x", "core")
    grid = Mesh(mesh.devices.reshape(NZ, NY, NX, 2), axes)
    rows, cols = axes[:2], axes[2:]
    return jax.shard_map(
        steps,
        mesh=grid,
        in_specs=(P(rows, cols), P(rows, cols), P(rows, cols), P(rows, cols, None), P(cols, None)),
        out_specs=P(cols, rows),
        check_vma=False,
    )
```

```python
import math

import jax
import jax.numpy as jnp
from jax import lax
from jax.experimental import pallas as pl
from jax.experimental.pallas import tpu as pltpu
from jax.sharding import Mesh, PartitionSpec as P


HD = 128
HEADS = 4
HALF = HEADS * HD
TOP = 3
NZ, NY, NX = 16, 4, 4
TOK = 384
SL = TOK // NY
EXT = HALF + 16
LOG2E = 1.4426950408889634
COEF = LOG2E / math.sqrt(HD)
DEAD = -1e30
NONE = NZ * NY
HOPS = NZ // 2
SLOTS = tuple(2 * d if d < HOPS else 2 * (NZ - d) - 1 for d in range(NZ))


def pallas(mib, kernel, **kw):
    grant = pltpu.CompilerParams(vmem_limit_bytes=mib * 1024 * 1024)
    return pl.pallas_call(kernel, compiler_params=grant, **kw)


def send(a, axis, s):
    n = lax.axis_size(axis)
    return lax.ppermute(a, axis, [(i, (i + s) % n) for i in range(n)])


def ahead(k):
    return [(i, i + 1) for i in range(k - 1, NZ - 1)]


def astern(k):
    return [((r - k + 1) % NZ, (r - k) % NZ) for r in range(HOPS - 1)]


def tn(a, b):
    return lax.dot_general(a, b, (((0,), (0,)), ((), ())), preferred_element_type=jnp.float32)


def pack_kernel(k_ref, v_ref, out_ref):
    for y in range(NY):
        out_ref[y, :, :HD] = k_ref[y * SL : (y + 1) * SL, :]
        out_ref[y, :, HD:] = v_ref[y * SL : (y + 1) * SL, :]


def own_kernel(code_ref, q_ref, k_ref, v_ref, qx_ref, o_ref, lse_ref):
    keep = lax.broadcasted_iota(jnp.int32, (TOK, TOK), 0) <= lax.broadcasted_iota(
        jnp.int32, (TOK, TOK), 1
    )
    k = k_ref[...]
    v = v_ref[...]
    rows = []
    for h in range(HEADS):
        q = q_ref[:, h * HD : (h + 1) * HD].T
        qx_ref[h * HD : (h + 1) * HD, :] = q
        s = jnp.dot(k, q, preferred_element_type=jnp.float32)
        s = jnp.where(keep, s * COEF, DEAD)
        top = jnp.max(s, axis=0, keepdims=True)
        p = jnp.exp2(s - top)
        total = jnp.sum(p, axis=0, keepdims=True)
        o = tn(v, p.astype(jnp.bfloat16)) * (1.0 / total)
        o_ref[h * HD : (h + 1) * HD, :] = o.astype(jnp.bfloat16)
        rows.append(top + jnp.log2(total))
    lse_ref[...] = jnp.concatenate(rows + rows, axis=0)
    lane = lax.broadcasted_iota(jnp.int32, (16, TOK), 1)
    codes = jnp.zeros((16, TOK), jnp.float32)
    for i in range(HEADS * TOP):
        codes = jnp.where(lane == i, code_ref[i].astype(jnp.float32), codes)
    qx_ref[HALF:, :] = codes.astype(jnp.bfloat16)


def slices_of(code_ref, kv_ref, q_ref, o_ref, base):
    rows = []
    for h in range(HEADS):
        codes = [code_ref[base + h * TOP + j] for j in range(TOP)]
        picked = [kv_ref[jnp.minimum(c, NONE - 1)] for c in codes]
        bias = [jnp.where(c < NONE, 0.0, DEAD).astype(jnp.float32) for c in codes]
        k = jnp.concatenate([t[:, :HD] for t in picked], axis=0)
        v = jnp.concatenate([t[:, HD:] for t in picked], axis=0)
        s = jnp.dot(k, q_ref[h * HD : (h + 1) * HD, :], preferred_element_type=jnp.float32)
        s = [s[j * SL : (j + 1) * SL] * COEF + bias[j] for j in range(TOP)]
        s = jnp.concatenate(s, axis=0)
        top = jnp.max(s, axis=0, keepdims=True)
        p = jnp.exp2(s - top)
        total = jnp.sum(p, axis=0, keepdims=True)
        o = tn(v, p.astype(jnp.bfloat16)) * (1.0 / total)
        o_ref[h * HD : (h + 1) * HD, :] = o.astype(jnp.bfloat16)
        lse = top + jnp.log2(total)
        hi = lse.astype(jnp.bfloat16).astype(jnp.float32)
        mid = (lse - hi).astype(jnp.bfloat16).astype(jnp.float32)
        rows += [hi, mid, lse - hi - mid]
    rows += [jnp.zeros((4, TOK), jnp.float32)]
    o_ref[HALF:, :] = jnp.concatenate(rows, axis=0).astype(jnp.bfloat16)


def slices_kernel(code_ref, kv_ref, *rest):
    n = len(rest) // 2
    for i in range(n):
        slices_of(code_ref, kv_ref, rest[i], rest[n + i], i * HEADS * TOP)


def merge_kernel(own_ref, lse_ref, p0, p1, p2, p3, out_ref):
    parts = (p0, p1, p2, p3)
    tails = [p[HALF:, :].astype(jnp.float32) for p in parts]
    for h in range(HEADS):
        span = slice(h * HD, (h + 1) * HD)
        own = lse_ref[h : h + 1, :]
        lses = [
            t[3 * h : 3 * h + 1] + t[3 * h + 1 : 3 * h + 2] + t[3 * h + 2 : 3 * h + 3]
            for t in tails
        ]
        top = own
        for x in lses:
            top = jnp.maximum(top, x)
        w = jnp.exp2(own - top)
        total = w
        acc = w * own_ref[span, :].astype(jnp.float32)
        for p, x in zip(parts, lses):
            w = jnp.exp2(x - top)
            total = total + w
            acc = acc + w * p[span, :].astype(jnp.float32)
        out_ref[span, :] = (acc * (1.0 / total)).astype(jnp.bfloat16)


def turn_kernel(cols_ref, mine_ref, got_ref, out_ref, blocks, turned, sems, out_sems):
    loads = []
    for s in range(NX):
        cols = pl.ds(pl.multiple_of(cols_ref[s] * HALF, HALF), HALF)
        for i, src in enumerate((mine_ref, got_ref)):
            at = 2 * s + i
            loads.append(pltpu.make_async_copy(src.at[:, cols], blocks.at[at], sems.at[at]))
    for load in loads:
        load.start()
    stores = []
    for s in range(NX):
        for i in range(2):
            loads[2 * s + i].wait()
            turned[s, :, i * HALF : (i + 1) * HALF] = blocks[2 * s + i].T
        stores.append(pltpu.make_async_copy(turned.at[s], out_ref.at[s], out_sems.at[s]))
        stores[s].start()
    for store in stores:
        store.wait()


def piece_of(w_ref, s, mine_ref, got_ref):
    out = jnp.dot(w_ref[s, :, :HALF], mine_ref[...], preferred_element_type=jnp.float32)
    return out + jnp.dot(w_ref[s, :, HALF:], got_ref[...], preferred_element_type=jnp.float32)


def pieces_kernel(w_ref, mine_ref, got_ref, *outs):
    for s, out in zip((2, 1, 3), outs):
        out[...] = piece_of(w_ref, s, mine_ref, got_ref).astype(jnp.bfloat16)


def mine_kernel(w_ref, mine_ref, got_ref, out_ref):
    out_ref[...] = piece_of(w_ref, 0, mine_ref, got_ref)


def sum_kernel(mine_ref, g1, g2, g3, out_ref):
    out = mine_ref[...]
    for g in (g1, g2, g3):
        out += g[...].astype(jnp.float32)
    out_ref[...] = out.astype(jnp.bfloat16)


def bf16(*shape):
    return jax.ShapeDtypeStruct(shape, jnp.bfloat16)


def f32(*shape):
    return jax.ShapeDtypeStruct(shape, jnp.float32)


def steps(queries, keys, values, block_ids, out_weight):
    z = lax.axis_index("z")
    y = lax.axis_index("y")
    x = lax.axis_index("x")
    core = lax.axis_index("core")
    vmem = pl.BlockSpec(memory_space=pltpu.VMEM)
    smem = pl.BlockSpec(memory_space=pltpu.SMEM)
    packed = pallas(
        4, pack_kernel, in_specs=[vmem] * 2, out_specs=vmem, out_shape=bf16(NY, SL, 2 * HD)
    )(keys, values)
    row = lax.all_to_all(packed, "y", 0, 0)
    ids = block_ids.reshape(HEADS * TOP)
    slot = jnp.zeros_like(ids)
    offset = (ids // NY - z) % NZ
    for d, place in enumerate(SLOTS):
        slot = jnp.where(offset == d, place, slot)
    code = jnp.where(ids < z * NY + y, slot * NY + ids % NY, NONE)
    kept = [row]
    p = m = row
    for k in range(1, HOPS + 1):
        p = lax.ppermute(p, "z", ahead(k))
        kept.append(p)
        if k < HOPS:
            m = lax.ppermute(m, "z", astern(k))
            kept.append(m)
    kv = jnp.concatenate(kept, axis=0)
    w_got = send(out_weight, "core", 1)
    qx, own, own_lse = pallas(
        8,
        own_kernel,
        in_specs=[smem] + [vmem] * 3,
        out_specs=[vmem] * 3,
        out_shape=[bf16(EXT, TOK), bf16(HALF, TOK), f32(2 * HEADS, TOK)],
    )(code, queries, keys, values)
    order = (2, 1, 3)
    qs = [send(qx, "y", s) for s in order]
    codes = jnp.stack([a[HALF, : HEADS * TOP] for a in qs], axis=0).astype(jnp.int32).reshape(-1)
    cols = (x + jnp.arange(NX, dtype=jnp.int32)) % NX * 2 + core
    w = pallas(
        12,
        turn_kernel,
        in_specs=[smem] + [pl.BlockSpec(memory_space=pltpu.HBM)] * 2,
        out_specs=pl.BlockSpec(memory_space=pltpu.HBM),
        out_shape=bf16(NX, HALF, 2 * HALF),
        scratch_shapes=[
            pltpu.VMEM((2 * NX, HALF, HALF), jnp.bfloat16),
            pltpu.VMEM((NX, HALF, 2 * HALF), jnp.bfloat16),
            pltpu.SemaphoreType.DMA((2 * NX,)),
            pltpu.SemaphoreType.DMA((NX,)),
        ],
    )(cols, out_weight, w_got)
    parts = pallas(
        12,
        slices_kernel,
        in_specs=[smem] + [vmem] * 4,
        out_specs=[vmem] * 3,
        out_shape=[bf16(EXT, TOK)] * 3,
    )(codes, kv, *qs)
    back = [send(o, "y", -s) for s, o in zip(order, parts)]
    (home,) = pallas(
        12,
        slices_kernel,
        in_specs=[smem] + [vmem] * 2,
        out_specs=[vmem],
        out_shape=[bf16(EXT, TOK)],
    )(code, kv, qx)
    att = pallas(
        8, merge_kernel, in_specs=[vmem] * 6, out_specs=vmem, out_shape=bf16(HALF, TOK)
    )(own, own_lse, home, *back)
    att_got = send(att, "core", 1)
    pieces = pallas(
        16,
        pieces_kernel,
        in_specs=[vmem] * 3,
        out_specs=[vmem] * 3,
        out_shape=[bf16(HALF, TOK)] * 3,
    )(w, att, att_got)
    got = [send(p, "x", s) for s, p in zip(order, pieces)]
    mine = pallas(
        12, mine_kernel, in_specs=[vmem] * 3, out_specs=vmem, out_shape=f32(HALF, TOK)
    )(w, att, att_got)
    return pallas(
        8, sum_kernel, in_specs=[vmem] * 4, out_specs=vmem, out_shape=bf16(HALF, TOK)
    )(mine, *got)


def solution(mesh):
    axes = ("z", "y", "x", "core")
    grid = Mesh(mesh.devices.reshape(NZ, NY, NX, 2), axes)
    rows, cols = axes[:2], axes[2:]
    return jax.shard_map(
        steps,
        mesh=grid,
        in_specs=(P(rows, cols), P(rows, cols), P(rows, cols), P(rows, cols, None), P(cols, None)),
        out_specs=P(cols, rows),
        check_vma=False,
    )
```

```python
import functools
import math

import jax
import jax.numpy as jnp
from jax import lax
from jax.experimental import pallas as pl
from jax.experimental.pallas import tpu as pltpu
from jax.sharding import Mesh, PartitionSpec as P


HD = 128
HEADS = 4
HALF = HEADS * HD
TOP = 3
NZ, NY, NX = 16, 4, 4
TOK = 384
SL = TOK // NY
EXT = HALF + 16
LOG2E = 1.4426950408889634
COEF = LOG2E / math.sqrt(HD)
DEAD = -1e30
NONE = NZ * NY
HOPS = NZ // 2
SLOTS = tuple(2 * d if d < HOPS else 2 * (NZ - d) - 1 for d in range(NZ))


def pallas(mib, kernel, **kw):
    grant = pltpu.CompilerParams(vmem_limit_bytes=mib * 1024 * 1024)
    return pl.pallas_call(kernel, compiler_params=grant, **kw)


def send(a, axis, s):
    n = lax.axis_size(axis)
    return lax.ppermute(a, axis, [(i, (i + s) % n) for i in range(n)])


def ahead(k):
    return [(i, i + 1) for i in range(k - 1, NZ - 1)]


def astern(k):
    return [((r - k + 1) % NZ, (r - k) % NZ) for r in range(HOPS - 1)]


def tn(a, b):
    return lax.dot_general(a, b, (((0,), (0,)), ((), ())), preferred_element_type=jnp.float32)


def pack_kernel(k_ref, v_ref, out_ref):
    for y in range(NY):
        out_ref[y, :, :HD] = k_ref[y * SL : (y + 1) * SL, :]
        out_ref[y, :, HD:] = v_ref[y * SL : (y + 1) * SL, :]


def own_kernel(code_ref, q_ref, k_ref, v_ref, qx_ref, o_ref, lse_ref):
    keep = lax.broadcasted_iota(jnp.int32, (TOK, TOK), 0) <= lax.broadcasted_iota(
        jnp.int32, (TOK, TOK), 1
    )
    k = k_ref[...]
    v = v_ref[...]
    rows = []
    for h in range(HEADS):
        q = q_ref[:, h * HD : (h + 1) * HD].T
        qx_ref[h * HD : (h + 1) * HD, :] = q
        s = jnp.dot(k, q, preferred_element_type=jnp.float32)
        s = jnp.where(keep, s * COEF, DEAD)
        top = jnp.max(s, axis=0, keepdims=True)
        p = jnp.exp2(s - top)
        total = jnp.sum(p, axis=0, keepdims=True)
        o = tn(v, p.astype(jnp.bfloat16)) * (1.0 / total)
        o_ref[h * HD : (h + 1) * HD, :] = o.astype(jnp.bfloat16)
        rows.append(top + jnp.log2(total))
    lse_ref[...] = jnp.concatenate(rows + rows, axis=0)
    lane = lax.broadcasted_iota(jnp.int32, (16, TOK), 1)
    codes = jnp.zeros((16, TOK), jnp.float32)
    for i in range(HEADS * TOP):
        codes = jnp.where(lane == i, code_ref[i].astype(jnp.float32), codes)
    qx_ref[HALF:, :] = codes.astype(jnp.bfloat16)


def slices_of(code_ref, kv_ref, q_ref, o_ref, base):
    rows = []
    for h in range(HEADS):
        codes = [code_ref[base + h * TOP + j] for j in range(TOP)]
        picked = [kv_ref[jnp.minimum(c, NONE - 1)] for c in codes]
        bias = [jnp.where(c < NONE, 0.0, DEAD).astype(jnp.float32) for c in codes]
        k = jnp.concatenate([t[:, :HD] for t in picked], axis=0)
        v = jnp.concatenate([t[:, HD:] for t in picked], axis=0)
        s = jnp.dot(k, q_ref[h * HD : (h + 1) * HD, :], preferred_element_type=jnp.float32)
        s = [s[j * SL : (j + 1) * SL] * COEF + bias[j] for j in range(TOP)]
        s = jnp.concatenate(s, axis=0)
        top = jnp.max(s, axis=0, keepdims=True)
        p = jnp.exp2(s - top)
        total = jnp.sum(p, axis=0, keepdims=True)
        o = tn(v, p.astype(jnp.bfloat16)) * (1.0 / total)
        o_ref[h * HD : (h + 1) * HD, :] = o.astype(jnp.bfloat16)
        lse = top + jnp.log2(total)
        hi = lse.astype(jnp.bfloat16).astype(jnp.float32)
        mid = (lse - hi).astype(jnp.bfloat16).astype(jnp.float32)
        rows += [hi, mid, lse - hi - mid]
    rows += [jnp.zeros((4, TOK), jnp.float32)]
    o_ref[HALF:, :] = jnp.concatenate(rows, axis=0).astype(jnp.bfloat16)


def slices_kernel(code_ref, kv_ref, q_ref, o_ref, *, base):
    slices_of(code_ref, kv_ref, q_ref, o_ref, base)


def merge_kernel(own_ref, lse_ref, p0, p1, p2, p3, out_ref):
    parts = (p0, p1, p2, p3)
    tails = [p[HALF:, :].astype(jnp.float32) for p in parts]
    for h in range(HEADS):
        span = slice(h * HD, (h + 1) * HD)
        own = lse_ref[h : h + 1, :]
        lses = [
            t[3 * h : 3 * h + 1] + t[3 * h + 1 : 3 * h + 2] + t[3 * h + 2 : 3 * h + 3]
            for t in tails
        ]
        top = own
        for x in lses:
            top = jnp.maximum(top, x)
        w = jnp.exp2(own - top)
        total = w
        acc = w * own_ref[span, :].astype(jnp.float32)
        for p, x in zip(parts, lses):
            w = jnp.exp2(x - top)
            total = total + w
            acc = acc + w * p[span, :].astype(jnp.float32)
        out_ref[span, :] = (acc * (1.0 / total)).astype(jnp.bfloat16)


def turn_kernel(cols_ref, mine_ref, got_ref, out_ref, blocks, turned, sems, out_sems):
    loads = []
    for s in range(NX):
        cols = pl.ds(pl.multiple_of(cols_ref[s] * HALF, HALF), HALF)
        for i, src in enumerate((mine_ref, got_ref)):
            at = 2 * s + i
            loads.append(pltpu.make_async_copy(src.at[:, cols], blocks.at[at], sems.at[at]))
    for load in loads:
        load.start()
    stores = []
    for s in range(NX):
        for i in range(2):
            loads[2 * s + i].wait()
            turned[s, :, i * HALF : (i + 1) * HALF] = blocks[2 * s + i].T
        stores.append(pltpu.make_async_copy(turned.at[s], out_ref.at[s], out_sems.at[s]))
        stores[s].start()
    for store in stores:
        store.wait()


def piece_of(w_ref, s, mine_ref, got_ref):
    out = jnp.dot(w_ref[s, :, :HALF], mine_ref[...], preferred_element_type=jnp.float32)
    return out + jnp.dot(w_ref[s, :, HALF:], got_ref[...], preferred_element_type=jnp.float32)


def piece_kernel(w_ref, mine_ref, got_ref, out_ref, *, s):
    out_ref[...] = piece_of(w_ref, s, mine_ref, got_ref).astype(jnp.bfloat16)


def mine_kernel(w_ref, mine_ref, got_ref, out_ref):
    out_ref[...] = piece_of(w_ref, 0, mine_ref, got_ref)


def sum_kernel(mine_ref, g1, g2, g3, out_ref):
    out = mine_ref[...]
    for g in (g1, g2, g3):
        out += g[...].astype(jnp.float32)
    out_ref[...] = out.astype(jnp.bfloat16)


def bf16(*shape):
    return jax.ShapeDtypeStruct(shape, jnp.bfloat16)


def f32(*shape):
    return jax.ShapeDtypeStruct(shape, jnp.float32)


def steps(queries, keys, values, block_ids, out_weight):
    z = lax.axis_index("z")
    y = lax.axis_index("y")
    x = lax.axis_index("x")
    core = lax.axis_index("core")
    vmem = pl.BlockSpec(memory_space=pltpu.VMEM)
    smem = pl.BlockSpec(memory_space=pltpu.SMEM)
    packed = pallas(
        60, pack_kernel, in_specs=[vmem] * 2, out_specs=vmem, out_shape=bf16(NY, SL, 2 * HD)
    )(keys, values)
    row = lax.all_to_all(packed, "y", 0, 0)
    ids = block_ids.reshape(HEADS * TOP)
    slot = jnp.zeros_like(ids)
    offset = (ids // NY - z) % NZ
    for d, place in enumerate(SLOTS):
        slot = jnp.where(offset == d, place, slot)
    code = jnp.where(ids < z * NY + y, slot * NY + ids % NY, NONE)
    kept = [row]
    p = m = row
    for k in range(1, HOPS + 1):
        p = lax.ppermute(p, "z", ahead(k))
        kept.append(p)
        if k < HOPS:
            m = lax.ppermute(m, "z", astern(k))
            kept.append(m)
    w_got = send(out_weight, "core", 1)
    qx, own, own_lse = pallas(
        8,
        own_kernel,
        in_specs=[smem] + [vmem] * 3,
        out_specs=[vmem] * 3,
        out_shape=[bf16(EXT, TOK), bf16(HALF, TOK), f32(2 * HEADS, TOK)],
    )(code, queries, keys, values)
    order = (2, 1, 3)
    qs = [send(qx, "y", s) for s in order]
    codes = jnp.stack([a[HALF, : HEADS * TOP] for a in qs], axis=0).astype(jnp.int32).reshape(-1)
    cols = (x + jnp.arange(NX, dtype=jnp.int32)) % NX * 2 + core
    w = pallas(
        12,
        turn_kernel,
        in_specs=[smem] + [pl.BlockSpec(memory_space=pltpu.HBM)] * 2,
        out_specs=pl.BlockSpec(memory_space=pltpu.HBM),
        out_shape=bf16(NX, HALF, 2 * HALF),
        scratch_shapes=[
            pltpu.VMEM((2 * NX, HALF, HALF), jnp.bfloat16),
            pltpu.VMEM((NX, HALF, 2 * HALF), jnp.bfloat16),
            pltpu.SemaphoreType.DMA((2 * NX,)),
            pltpu.SemaphoreType.DMA((NX,)),
        ],
    )(cols, out_weight, w_got)
    kv = jnp.concatenate(kept, axis=0)

    def attend(code, q, base):
        return pallas(
            12,
            functools.partial(slices_kernel, base=base),
            in_specs=[smem] + [vmem] * 2,
            out_specs=vmem,
            out_shape=bf16(EXT, TOK),
        )(code, kv, q)

    back = []
    for i, s in enumerate(order):
        part = attend(codes, qs[i], i * HEADS * TOP)
        back.append(send(part, "y", -s))
    home = attend(code, qx, 0)
    att = pallas(
        8, merge_kernel, in_specs=[vmem] * 6, out_specs=vmem, out_shape=bf16(HALF, TOK)
    )(own, own_lse, home, *back)
    att_got = send(att, "core", 1)
    got = []
    for s in order:
        part = pallas(
            12,
            functools.partial(piece_kernel, s=s),
            in_specs=[vmem] * 3,
            out_specs=vmem,
            out_shape=bf16(HALF, TOK),
        )(w, att, att_got)
        got.append(send(part, "x", s))
    mine = pallas(
        12, mine_kernel, in_specs=[vmem] * 3, out_specs=vmem, out_shape=f32(HALF, TOK)
    )(w, att, att_got)
    return pallas(
        8, sum_kernel, in_specs=[vmem] * 4, out_specs=vmem, out_shape=bf16(HALF, TOK)
    )(mine, *got)


def solution(mesh):
    axes = ("z", "y", "x", "core")
    grid = Mesh(mesh.devices.reshape(NZ, NY, NX, 2), axes)
    rows, cols = axes[:2], axes[2:]
    return jax.shard_map(
        steps,
        mesh=grid,
        in_specs=(P(rows, cols), P(rows, cols), P(rows, cols), P(rows, cols, None), P(cols, None)),
        out_specs=P(cols, rows),
        check_vma=False,
    )
```

```python
import functools
import math

import jax
import jax.numpy as jnp
from jax import lax
from jax.experimental import pallas as pl
from jax.experimental.pallas import tpu as pltpu
from jax.sharding import Mesh, PartitionSpec as P


HD = 128
HEADS = 4
HALF = HEADS * HD
TOP = 3
NZ, NY, NX = 16, 4, 4
TOK = 384
SL = TOK // NY
EXT = HALF + 16
LOG2E = 1.4426950408889634
COEF = LOG2E / math.sqrt(HD)
DEAD = -1e30
NONE = NZ * NY
HOPS = NZ // 2
SLOTS = tuple(2 * d if d < HOPS else 2 * (NZ - d) - 1 for d in range(NZ))


def pallas(mib, kernel, **kw):
    grant = pltpu.CompilerParams(vmem_limit_bytes=mib * 1024 * 1024)
    return pl.pallas_call(kernel, compiler_params=grant, **kw)


def send(a, axis, s):
    n = lax.axis_size(axis)
    return lax.ppermute(a, axis, [(i, (i + s) % n) for i in range(n)])


def ahead(k):
    return [(i, i + 1) for i in range(k - 1, NZ - 1)]


def astern(k):
    return [((r - k + 1) % NZ, (r - k) % NZ) for r in range(HOPS - 1)]


def tn(a, b):
    return lax.dot_general(a, b, (((0,), (0,)), ((), ())), preferred_element_type=jnp.float32)


def pack_kernel(k_ref, v_ref, out_ref):
    for y in range(NY):
        out_ref[y, :, :HD] = k_ref[y * SL : (y + 1) * SL, :]
        out_ref[y, :, HD:] = v_ref[y * SL : (y + 1) * SL, :]


def query_kernel(code_ref, q_ref, out_ref):
    lane = lax.broadcasted_iota(jnp.int32, (16, TOK), 1)
    codes = jnp.zeros((16, TOK), jnp.float32)
    for i in range(HEADS * TOP):
        codes = jnp.where(lane == i, code_ref[i].astype(jnp.float32), codes)
    codes = codes.astype(jnp.bfloat16)
    for h in range(HEADS):
        q = q_ref[:, h * HD : (h + 1) * HD].T
        for y in range(NY):
            out_ref[y, h * HD : (h + 1) * HD, :] = q
    for y in range(NY):
        out_ref[y, HALF:, :] = codes


def own_kernel(q_ref, k_ref, v_ref, o_ref, lse_ref):
    keep = lax.broadcasted_iota(jnp.int32, (TOK, TOK), 0) <= lax.broadcasted_iota(
        jnp.int32, (TOK, TOK), 1
    )
    k = k_ref[...]
    v = v_ref[...]
    rows = []
    for h in range(HEADS):
        q = q_ref[:, h * HD : (h + 1) * HD].T
        s = jnp.dot(k, q, preferred_element_type=jnp.float32)
        s = jnp.where(keep, s * COEF, DEAD)
        top = jnp.max(s, axis=0, keepdims=True)
        p = jnp.exp2(s - top)
        total = jnp.sum(p, axis=0, keepdims=True)
        o = tn(v, p.astype(jnp.bfloat16)) * (1.0 / total)
        o_ref[h * HD : (h + 1) * HD, :] = o.astype(jnp.bfloat16)
        rows.append(top + jnp.log2(total))
    lse_ref[...] = jnp.concatenate(rows + rows, axis=0)


def first_kernel(row_ref, out_ref, sem):
    copy = pltpu.make_async_copy(row_ref, out_ref.at[pl.ds(0, NY)], sem.at[0])
    copy.start()
    copy.wait()


def slices_kernel(home_ref, code_ref, kv_ref, q_ref, o_ref, *, s):
    base = home_ref[s] * HEADS * TOP
    rows = []
    for h in range(HEADS):
        codes = [code_ref[base + h * TOP + j] for j in range(TOP)]
        picked = [kv_ref[jnp.minimum(c, NONE - 1)] for c in codes]
        bias = [jnp.where(c < NONE, 0.0, DEAD).astype(jnp.float32) for c in codes]
        k = jnp.concatenate([t[:, :HD] for t in picked], axis=0)
        v = jnp.concatenate([t[:, HD:] for t in picked], axis=0)
        t = jnp.dot(k, q_ref[h * HD : (h + 1) * HD, :], preferred_element_type=jnp.float32)
        t = [t[j * SL : (j + 1) * SL] * COEF + bias[j] for j in range(TOP)]
        t = jnp.concatenate(t, axis=0)
        top = jnp.max(t, axis=0, keepdims=True)
        p = jnp.exp2(t - top)
        total = jnp.sum(p, axis=0, keepdims=True)
        o = tn(v, p.astype(jnp.bfloat16)) * (1.0 / total)
        o_ref[h * HD : (h + 1) * HD, :] = o.astype(jnp.bfloat16)
        lse = top + jnp.log2(total)
        hi = lse.astype(jnp.bfloat16).astype(jnp.float32)
        mid = (lse - hi).astype(jnp.bfloat16).astype(jnp.float32)
        rows += [hi, mid, lse - hi - mid]
    rows += [jnp.zeros((4, TOK), jnp.float32)]
    o_ref[HALF:, :] = jnp.concatenate(rows, axis=0).astype(jnp.bfloat16)


def merge_kernel(own_ref, lse_ref, p0, p1, p2, p3, out_ref):
    parts = (p0, p1, p2, p3)
    tails = [p[HALF:, :].astype(jnp.float32) for p in parts]
    for h in range(HEADS):
        span = slice(h * HD, (h + 1) * HD)
        own = lse_ref[h : h + 1, :]
        lses = [
            t[3 * h : 3 * h + 1] + t[3 * h + 1 : 3 * h + 2] + t[3 * h + 2 : 3 * h + 3]
            for t in tails
        ]
        top = own
        for x in lses:
            top = jnp.maximum(top, x)
        w = jnp.exp2(own - top)
        total = w
        acc = w * own_ref[span, :].astype(jnp.float32)
        for p, x in zip(parts, lses):
            w = jnp.exp2(x - top)
            total = total + w
            acc = acc + w * p[span, :].astype(jnp.float32)
        out_ref[span, :] = (acc * (1.0 / total)).astype(jnp.bfloat16)


def turn_kernel(cols_ref, mine_ref, got_ref, out_ref, blocks, turned, sems, out_sems):
    loads = []
    for s in range(NX):
        cols = pl.ds(pl.multiple_of(cols_ref[s] * HALF, HALF), HALF)
        for i, src in enumerate((mine_ref, got_ref)):
            at = 2 * s + i
            loads.append(pltpu.make_async_copy(src.at[:, cols], blocks.at[at], sems.at[at]))
    for load in loads:
        load.start()
    stores = []
    for s in range(NX):
        for i in range(2):
            loads[2 * s + i].wait()
            turned[s, :, i * HALF : (i + 1) * HALF] = blocks[2 * s + i].T
        stores.append(pltpu.make_async_copy(turned.at[s], out_ref.at[s], out_sems.at[s]))
        stores[s].start()
    for store in stores:
        store.wait()


def piece_of(w_ref, s, mine_ref, got_ref):
    out = jnp.dot(w_ref[s, :, :HALF], mine_ref[...], preferred_element_type=jnp.float32)
    return out + jnp.dot(w_ref[s, :, HALF:], got_ref[...], preferred_element_type=jnp.float32)


def piece_kernel(w_ref, mine_ref, got_ref, out_ref, *, s):
    out_ref[...] = piece_of(w_ref, s, mine_ref, got_ref).astype(jnp.bfloat16)


def mine_kernel(w_ref, mine_ref, got_ref, out_ref):
    out_ref[...] = piece_of(w_ref, 0, mine_ref, got_ref)


def sum_kernel(mine_ref, g1, g2, g3, out_ref):
    out = mine_ref[...]
    for g in (g1, g2, g3):
        out += g[...].astype(jnp.float32)
    out_ref[...] = out.astype(jnp.bfloat16)


def bf16(*shape):
    return jax.ShapeDtypeStruct(shape, jnp.bfloat16)


def f32(*shape):
    return jax.ShapeDtypeStruct(shape, jnp.float32)


def steps(queries, keys, values, block_ids, out_weight):
    z = lax.axis_index("z")
    y = lax.axis_index("y")
    x = lax.axis_index("x")
    core = lax.axis_index("core")
    vmem = pl.BlockSpec(memory_space=pltpu.VMEM)
    smem = pl.BlockSpec(memory_space=pltpu.SMEM)
    packed = pallas(
        60, pack_kernel, in_specs=[vmem] * 2, out_specs=vmem, out_shape=bf16(NY, SL, 2 * HD)
    )(keys, values)
    row = lax.all_to_all(packed, "y", 0, 0)
    ids = block_ids.reshape(HEADS * TOP)
    slot = jnp.zeros_like(ids)
    offset = (ids // NY - z) % NZ
    for d, place in enumerate(SLOTS):
        slot = jnp.where(offset == d, place, slot)
    code = jnp.where(ids < z * NY + y, slot * NY + ids % NY, NONE)
    anyw = pl.BlockSpec(memory_space=pl.ANY)
    kv = pallas(
        2,
        first_kernel,
        in_specs=[anyw],
        out_specs=anyw,
        out_shape=bf16(NZ * NY, SL, 2 * HD),
        scratch_shapes=[pltpu.SemaphoreType.DMA((1,))],
    )(row)

    def put(kv, a, at):
        return lax.dynamic_update_slice(kv, a, (at * NY, 0, 0))

    p = m = row
    for k in range(1, HOPS + 1):
        p = lax.ppermute(p, "z", ahead(k))
        kv = put(kv, p, 2 * k - 1)
        if k < HOPS:
            m = lax.ppermute(m, "z", astern(k))
            kv = put(kv, m, 2 * k)
    qx = pallas(
        60, query_kernel, in_specs=[smem, vmem], out_specs=vmem, out_shape=bf16(NY, EXT, TOK)
    )(code, queries)
    qs = lax.all_to_all(qx, "y", 0, 0)
    own, own_lse = pallas(
        8,
        own_kernel,
        in_specs=[vmem] * 3,
        out_specs=[vmem] * 2,
        out_shape=[bf16(HALF, TOK), f32(2 * HEADS, TOK)],
    )(queries, keys, values)
    w_got = send(out_weight, "core", 1)
    codes = qs[:, HALF, : HEADS * TOP].astype(jnp.int32).reshape(-1)
    order = (2, 1, 3)
    cols = (x + jnp.arange(NX, dtype=jnp.int32)) % NX * 2 + core
    w = pallas(
        12,
        turn_kernel,
        in_specs=[smem] + [pl.BlockSpec(memory_space=pltpu.HBM)] * 2,
        out_specs=pl.BlockSpec(memory_space=pltpu.HBM),
        out_shape=bf16(NX, HALF, 2 * HALF),
        scratch_shapes=[
            pltpu.VMEM((2 * NX, HALF, HALF), jnp.bfloat16),
            pltpu.VMEM((NX, HALF, 2 * HALF), jnp.bfloat16),
            pltpu.SemaphoreType.DMA((2 * NX,)),
            pltpu.SemaphoreType.DMA((NX,)),
        ],
    )(cols, out_weight, w_got)
    homes = (y - jnp.arange(NY, dtype=jnp.int32)) % NY

    def attend(s):
        q = lax.dynamic_index_in_dim(qs, homes[s], keepdims=False)
        return pallas(
            12,
            functools.partial(slices_kernel, s=s),
            in_specs=[smem] * 2 + [vmem] * 2,
            out_specs=vmem,
            out_shape=bf16(EXT, TOK),
        )(homes, codes, kv, q)

    back = [send(attend(s), "y", -s) for s in order]
    home = attend(0)
    att = pallas(
        8, merge_kernel, in_specs=[vmem] * 6, out_specs=vmem, out_shape=bf16(HALF, TOK)
    )(own, own_lse, home, *back)
    att_got = send(att, "core", 1)
    got = []
    for s in order:
        part = pallas(
            12,
            functools.partial(piece_kernel, s=s),
            in_specs=[vmem] * 3,
            out_specs=vmem,
            out_shape=bf16(HALF, TOK),
        )(w, att, att_got)
        got.append(send(part, "x", s))
    mine = pallas(
        12, mine_kernel, in_specs=[vmem] * 3, out_specs=vmem, out_shape=f32(HALF, TOK)
    )(w, att, att_got)
    return pallas(
        8, sum_kernel, in_specs=[vmem] * 4, out_specs=vmem, out_shape=bf16(HALF, TOK)
    )(mine, *got)


def solution(mesh):
    axes = ("z", "y", "x", "core")
    grid = Mesh(mesh.devices.reshape(NZ, NY, NX, 2), axes)
    rows, cols = axes[:2], axes[2:]
    return jax.shard_map(
        steps,
        mesh=grid,
        in_specs=(P(rows, cols), P(rows, cols), P(rows, cols), P(rows, cols, None), P(cols, None)),
        out_specs=P(cols, rows),
        check_vma=False,
    )
```

```python
import functools
import math

import jax
import jax.numpy as jnp
from jax import lax
from jax.experimental import pallas as pl
from jax.experimental.pallas import tpu as pltpu
from jax.sharding import Mesh, PartitionSpec as P


HD = 128
HEADS = 4
HALF = HEADS * HD
TOP = 3
NZ, NY, NX = 16, 4, 4
TOK = 384
SL = TOK // NY
EXT = HALF + 16
LOG2E = 1.4426950408889634
COEF = LOG2E / math.sqrt(HD)
DEAD = -1e30
NONE = NZ * NY
HOPS = NZ // 2
SLOTS = tuple(2 * d if d < HOPS else 2 * (NZ - d) - 1 for d in range(NZ))


def pallas(mib, kernel, **kw):
    grant = pltpu.CompilerParams(vmem_limit_bytes=mib * 1024 * 1024)
    return pl.pallas_call(kernel, compiler_params=grant, **kw)


def send(a, axis, s):
    n = lax.axis_size(axis)
    return lax.ppermute(a, axis, [(i, (i + s) % n) for i in range(n)])


def ahead(k):
    return [(i, i + 1) for i in range(k - 1, NZ - 1)]


def astern(k):
    return [((r - k + 1) % NZ, (r - k) % NZ) for r in range(HOPS - 1)]


def tn(a, b):
    return lax.dot_general(a, b, (((0,), (0,)), ((), ())), preferred_element_type=jnp.float32)


def pack_kernel(k_ref, v_ref, out_ref):
    for y in range(NY):
        out_ref[y, :, :HD] = k_ref[y * SL : (y + 1) * SL, :]
        out_ref[y, :, HD:] = v_ref[y * SL : (y + 1) * SL, :]


def query_kernel(code_ref, q_ref, out_ref):
    lane = lax.broadcasted_iota(jnp.int32, (16, TOK), 1)
    codes = jnp.zeros((16, TOK), jnp.float32)
    for i in range(HEADS * TOP):
        codes = jnp.where(lane == i, code_ref[i].astype(jnp.float32), codes)
    codes = codes.astype(jnp.bfloat16)
    for h in range(HEADS):
        q = q_ref[:, h * HD : (h + 1) * HD].T
        for y in range(NY):
            out_ref[y, h * HD : (h + 1) * HD, :] = q
    for y in range(NY):
        out_ref[y, HALF:, :] = codes


def own_kernel(q_ref, k_ref, v_ref, o_ref, lse_ref):
    keep = lax.broadcasted_iota(jnp.int32, (TOK, TOK), 0) <= lax.broadcasted_iota(
        jnp.int32, (TOK, TOK), 1
    )
    k = k_ref[...]
    v = v_ref[...]
    rows = []
    for h in range(HEADS):
        q = q_ref[:, h * HD : (h + 1) * HD].T
        s = jnp.dot(k, q, preferred_element_type=jnp.float32)
        s = jnp.where(keep, s * COEF, DEAD)
        top = jnp.max(s, axis=0, keepdims=True)
        p = jnp.exp2(s - top)
        total = jnp.sum(p, axis=0, keepdims=True)
        o = tn(v, p.astype(jnp.bfloat16)) * (1.0 / total)
        o_ref[h * HD : (h + 1) * HD, :] = o.astype(jnp.bfloat16)
        rows.append(top + jnp.log2(total))
    lse_ref[...] = jnp.concatenate(rows + rows, axis=0)


def first_kernel(row_ref, out_ref, sem):
    copy = pltpu.make_async_copy(row_ref, out_ref.at[pl.ds(0, NY)], sem.at[0])
    copy.start()
    copy.wait()


def slices_kernel(home_ref, code_ref, kv_ref, q_ref, *outs, shifts):
    for s, o_ref in zip(shifts, outs):
        slices_of(home_ref[s], code_ref, kv_ref, q_ref, o_ref)


def slices_of(home, code_ref, kv_ref, q_ref, o_ref):
    base = home * HEADS * TOP
    rows = []
    for h in range(HEADS):
        codes = [code_ref[base + h * TOP + j] for j in range(TOP)]
        picked = [kv_ref[jnp.minimum(c, NONE - 1)] for c in codes]
        bias = [jnp.where(c < NONE, 0.0, DEAD).astype(jnp.float32) for c in codes]
        k = jnp.concatenate([t[:, :HD] for t in picked], axis=0)
        v = jnp.concatenate([t[:, HD:] for t in picked], axis=0)
        t = jnp.dot(k, q_ref[home, h * HD : (h + 1) * HD, :], preferred_element_type=jnp.float32)
        t = [t[j * SL : (j + 1) * SL] * COEF + bias[j] for j in range(TOP)]
        t = jnp.concatenate(t, axis=0)
        top = jnp.max(t, axis=0, keepdims=True)
        p = jnp.exp2(t - top)
        total = jnp.sum(p, axis=0, keepdims=True)
        o = tn(v, p.astype(jnp.bfloat16)) * (1.0 / total)
        o_ref[h * HD : (h + 1) * HD, :] = o.astype(jnp.bfloat16)
        lse = top + jnp.log2(total)
        hi = lse.astype(jnp.bfloat16).astype(jnp.float32)
        mid = (lse - hi).astype(jnp.bfloat16).astype(jnp.float32)
        rows += [hi, mid, lse - hi - mid]
    rows += [jnp.zeros((4, TOK), jnp.float32)]
    o_ref[HALF:, :] = jnp.concatenate(rows, axis=0).astype(jnp.bfloat16)


def merge_kernel(own_ref, lse_ref, p0, p1, p2, p3, out_ref):
    parts = (p0, p1, p2, p3)
    tails = [p[HALF:, :].astype(jnp.float32) for p in parts]
    for h in range(HEADS):
        span = slice(h * HD, (h + 1) * HD)
        own = lse_ref[h : h + 1, :]
        lses = [
            t[3 * h : 3 * h + 1] + t[3 * h + 1 : 3 * h + 2] + t[3 * h + 2 : 3 * h + 3]
            for t in tails
        ]
        top = own
        for x in lses:
            top = jnp.maximum(top, x)
        w = jnp.exp2(own - top)
        total = w
        acc = w * own_ref[span, :].astype(jnp.float32)
        for p, x in zip(parts, lses):
            w = jnp.exp2(x - top)
            total = total + w
            acc = acc + w * p[span, :].astype(jnp.float32)
        out_ref[span, :] = (acc * (1.0 / total)).astype(jnp.bfloat16)


def turn_kernel(cols_ref, mine_ref, got_ref, out_ref, blocks, turned, sems, out_sems):
    loads = []
    for s in range(NX):
        cols = pl.ds(pl.multiple_of(cols_ref[s] * HALF, HALF), HALF)
        for i, src in enumerate((mine_ref, got_ref)):
            at = 2 * s + i
            loads.append(pltpu.make_async_copy(src.at[:, cols], blocks.at[at], sems.at[at]))
    for load in loads:
        load.start()
    stores = []
    for s in range(NX):
        for i in range(2):
            loads[2 * s + i].wait()
            turned[s, :, i * HALF : (i + 1) * HALF] = blocks[2 * s + i].T
        stores.append(pltpu.make_async_copy(turned.at[s], out_ref.at[s], out_sems.at[s]))
        stores[s].start()
    for store in stores:
        store.wait()


def piece_of(w_ref, s, mine_ref, got_ref):
    out = jnp.dot(w_ref[s, :, :HALF], mine_ref[...], preferred_element_type=jnp.float32)
    return out + jnp.dot(w_ref[s, :, HALF:], got_ref[...], preferred_element_type=jnp.float32)


def piece_kernel(w_ref, mine_ref, got_ref, out_ref, *, s):
    out_ref[...] = piece_of(w_ref, s, mine_ref, got_ref).astype(jnp.bfloat16)


def mine_kernel(w_ref, mine_ref, got_ref, out_ref):
    out_ref[...] = piece_of(w_ref, 0, mine_ref, got_ref)


def sum_kernel(mine_ref, g1, g2, g3, out_ref):
    out = mine_ref[...]
    for g in (g1, g2, g3):
        out += g[...].astype(jnp.float32)
    out_ref[...] = out.astype(jnp.bfloat16)


def bf16(*shape):
    return jax.ShapeDtypeStruct(shape, jnp.bfloat16)


def f32(*shape):
    return jax.ShapeDtypeStruct(shape, jnp.float32)


def steps(queries, keys, values, block_ids, out_weight):
    z = lax.axis_index("z")
    y = lax.axis_index("y")
    x = lax.axis_index("x")
    core = lax.axis_index("core")
    vmem = pl.BlockSpec(memory_space=pltpu.VMEM)
    smem = pl.BlockSpec(memory_space=pltpu.SMEM)
    packed = pallas(
        60, pack_kernel, in_specs=[vmem] * 2, out_specs=vmem, out_shape=bf16(NY, SL, 2 * HD)
    )(keys, values)
    row = lax.all_to_all(packed, "y", 0, 0)
    ids = block_ids.reshape(HEADS * TOP)
    slot = jnp.zeros_like(ids)
    offset = (ids // NY - z) % NZ
    for d, place in enumerate(SLOTS):
        slot = jnp.where(offset == d, place, slot)
    code = jnp.where(ids < z * NY + y, slot * NY + ids % NY, NONE)
    anyw = pl.BlockSpec(memory_space=pl.ANY)
    kv = pallas(
        2,
        first_kernel,
        in_specs=[anyw],
        out_specs=anyw,
        out_shape=bf16(NZ * NY, SL, 2 * HD),
        scratch_shapes=[pltpu.SemaphoreType.DMA((1,))],
    )(row)

    def put(kv, a, at):
        return lax.dynamic_update_slice(kv, a, (at * NY, 0, 0))

    p = m = row
    for k in range(1, HOPS + 1):
        p = lax.ppermute(p, "z", ahead(k))
        kv = put(kv, p, 2 * k - 1)
        if k < HOPS:
            m = lax.ppermute(m, "z", astern(k))
            kv = put(kv, m, 2 * k)
    qx = pallas(
        60, query_kernel, in_specs=[smem, vmem], out_specs=vmem, out_shape=bf16(NY, EXT, TOK)
    )(code, queries)
    qs = lax.all_to_all(qx, "y", 0, 0)
    own, own_lse = pallas(
        8,
        own_kernel,
        in_specs=[vmem] * 3,
        out_specs=[vmem] * 2,
        out_shape=[bf16(HALF, TOK), f32(2 * HEADS, TOK)],
    )(queries, keys, values)
    w_got = send(out_weight, "core", 1)
    codes = qs[:, HALF, : HEADS * TOP].astype(jnp.int32).reshape(-1)
    order = (2, 1, 3)
    cols = (x + jnp.arange(NX, dtype=jnp.int32)) % NX * 2 + core
    w = pallas(
        12,
        turn_kernel,
        in_specs=[smem] + [pl.BlockSpec(memory_space=pltpu.HBM)] * 2,
        out_specs=pl.BlockSpec(memory_space=pltpu.HBM),
        out_shape=bf16(NX, HALF, 2 * HALF),
        scratch_shapes=[
            pltpu.VMEM((2 * NX, HALF, HALF), jnp.bfloat16),
            pltpu.VMEM((NX, HALF, 2 * HALF), jnp.bfloat16),
            pltpu.SemaphoreType.DMA((2 * NX,)),
            pltpu.SemaphoreType.DMA((NX,)),
        ],
    )(cols, out_weight, w_got)
    homes = (y - jnp.arange(NY, dtype=jnp.int32)) % NY

    def attend(shifts):
        return pallas(
            12,
            functools.partial(slices_kernel, shifts=shifts),
            in_specs=[smem] * 2 + [vmem] * 2,
            out_specs=[vmem] * len(shifts),
            out_shape=[bf16(EXT, TOK)] * len(shifts),
        )(homes, codes, kv, qs)

    parts = attend(order)
    back = [send(part, "y", -s) for s, part in zip(order, parts)]
    (home,) = attend((0,))
    att = pallas(
        8, merge_kernel, in_specs=[vmem] * 6, out_specs=vmem, out_shape=bf16(HALF, TOK)
    )(own, own_lse, home, *back)
    att_got = send(att, "core", 1)
    got = []
    for s in order:
        part = pallas(
            12,
            functools.partial(piece_kernel, s=s),
            in_specs=[vmem] * 3,
            out_specs=vmem,
            out_shape=bf16(HALF, TOK),
        )(w, att, att_got)
        got.append(send(part, "x", s))
    mine = pallas(
        12, mine_kernel, in_specs=[vmem] * 3, out_specs=vmem, out_shape=f32(HALF, TOK)
    )(w, att, att_got)
    return pallas(
        8, sum_kernel, in_specs=[vmem] * 4, out_specs=vmem, out_shape=bf16(HALF, TOK)
    )(mine, *got)


def solution(mesh):
    axes = ("z", "y", "x", "core")
    grid = Mesh(mesh.devices.reshape(NZ, NY, NX, 2), axes)
    rows, cols = axes[:2], axes[2:]
    return jax.shard_map(
        steps,
        mesh=grid,
        in_specs=(P(rows, cols), P(rows, cols), P(rows, cols), P(rows, cols, None), P(cols, None)),
        out_specs=P(cols, rows),
        check_vma=False,
    )
```

```python
import functools
import math

import jax
import jax.numpy as jnp
from jax import lax
from jax.experimental import pallas as pl
from jax.experimental.pallas import tpu as pltpu
from jax.sharding import Mesh, PartitionSpec as P


HD = 128
HEADS = 4
HALF = HEADS * HD
TOP = 3
NZ, NY, NX = 16, 4, 4
TOK = 384
SL = TOK // NY
EXT = HALF + 16
LOG2E = 1.4426950408889634
COEF = LOG2E / math.sqrt(HD)
DEAD = -1e30
NONE = NZ * NY
HOPS = NZ // 2
SLOTS = tuple(2 * d if d < HOPS else 2 * (NZ - d) - 1 for d in range(NZ))


def pallas(mib, kernel, **kw):
    grant = pltpu.CompilerParams(vmem_limit_bytes=mib * 1024 * 1024)
    return pl.pallas_call(kernel, compiler_params=grant, **kw)


def send(a, axis, s):
    n = lax.axis_size(axis)
    return lax.ppermute(a, axis, [(i, (i + s) % n) for i in range(n)])


def ahead(k):
    return [(i, i + 1) for i in range(k - 1, NZ - 1)]


def astern(k):
    return [((r - k + 1) % NZ, (r - k) % NZ) for r in range(HOPS - 1)]


def tn(a, b):
    return lax.dot_general(a, b, (((0,), (0,)), ((), ())), preferred_element_type=jnp.float32)


def pack_kernel(k_ref, v_ref, out_ref):
    for y in range(NY):
        out_ref[y, :, :HD] = k_ref[y * SL : (y + 1) * SL, :]
        out_ref[y, :, HD:] = v_ref[y * SL : (y + 1) * SL, :]


def query_kernel(code_ref, q_ref, qx_ref):
    for h in range(HEADS):
        qx_ref[h * HD : (h + 1) * HD, :] = q_ref[:, h * HD : (h + 1) * HD].T
    lane = lax.broadcasted_iota(jnp.int32, (16, TOK), 1)
    codes = jnp.zeros((16, TOK), jnp.float32)
    for i in range(HEADS * TOP):
        codes = jnp.where(lane == i, code_ref[i].astype(jnp.float32), codes)
    qx_ref[HALF:, :] = codes.astype(jnp.bfloat16)


def own_kernel(q_ref, k_ref, v_ref, o_ref, lse_ref):
    keep = lax.broadcasted_iota(jnp.int32, (TOK, TOK), 0) <= lax.broadcasted_iota(
        jnp.int32, (TOK, TOK), 1
    )
    k = k_ref[...]
    v = v_ref[...]
    rows = []
    for h in range(HEADS):
        q = q_ref[h * HD : (h + 1) * HD, :]
        s = jnp.dot(k, q, preferred_element_type=jnp.float32)
        s = jnp.where(keep, s * COEF, DEAD)
        top = jnp.max(s, axis=0, keepdims=True)
        p = jnp.exp2(s - top)
        total = jnp.sum(p, axis=0, keepdims=True)
        o = tn(v, p.astype(jnp.bfloat16)) * (1.0 / total)
        o_ref[h * HD : (h + 1) * HD, :] = o.astype(jnp.bfloat16)
        rows.append(top + jnp.log2(total))
    lse_ref[...] = jnp.concatenate(rows + rows, axis=0)


def slices_of(code_ref, kv_ref, q_ref, o_ref, base):
    rows = []
    for h in range(HEADS):
        codes = [code_ref[base + h * TOP + j] for j in range(TOP)]
        picked = [kv_ref[jnp.minimum(c, NONE - 1)] for c in codes]
        bias = [jnp.where(c < NONE, 0.0, DEAD).astype(jnp.float32) for c in codes]
        k = jnp.concatenate([t[:, :HD] for t in picked], axis=0)
        v = jnp.concatenate([t[:, HD:] for t in picked], axis=0)
        s = jnp.dot(k, q_ref[h * HD : (h + 1) * HD, :], preferred_element_type=jnp.float32)
        s = [s[j * SL : (j + 1) * SL] * COEF + bias[j] for j in range(TOP)]
        s = jnp.concatenate(s, axis=0)
        top = jnp.max(s, axis=0, keepdims=True)
        p = jnp.exp2(s - top)
        total = jnp.sum(p, axis=0, keepdims=True)
        o = tn(v, p.astype(jnp.bfloat16)) * (1.0 / total)
        o_ref[h * HD : (h + 1) * HD, :] = o.astype(jnp.bfloat16)
        lse = top + jnp.log2(total)
        hi = lse.astype(jnp.bfloat16).astype(jnp.float32)
        mid = (lse - hi).astype(jnp.bfloat16).astype(jnp.float32)
        rows += [hi, mid, lse - hi - mid]
    rows += [jnp.zeros((4, TOK), jnp.float32)]
    o_ref[HALF:, :] = jnp.concatenate(rows, axis=0).astype(jnp.bfloat16)


def slices_kernel(code_ref, kv_ref, *rest):
    n = len(rest) // 2
    for i in range(n):
        slices_of(code_ref, kv_ref, rest[i], rest[n + i], i * HEADS * TOP)


def merge_kernel(own_ref, lse_ref, p0, p1, p2, p3, out_ref):
    parts = (p0, p1, p2, p3)
    tails = [p[HALF:, :].astype(jnp.float32) for p in parts]
    for h in range(HEADS):
        span = slice(h * HD, (h + 1) * HD)
        own = lse_ref[h : h + 1, :]
        lses = [
            t[3 * h : 3 * h + 1] + t[3 * h + 1 : 3 * h + 2] + t[3 * h + 2 : 3 * h + 3]
            for t in tails
        ]
        top = own
        for x in lses:
            top = jnp.maximum(top, x)
        w = jnp.exp2(own - top)
        total = w
        acc = w * own_ref[span, :].astype(jnp.float32)
        for p, x in zip(parts, lses):
            w = jnp.exp2(x - top)
            total = total + w
            acc = acc + w * p[span, :].astype(jnp.float32)
        out_ref[span, :] = (acc * (1.0 / total)).astype(jnp.bfloat16)


def turn_kernel(cols_ref, mine_ref, got_ref, out_ref, blocks, turned, sems, out_sems):
    loads = []
    for s in range(NX):
        cols = pl.ds(pl.multiple_of(cols_ref[s] * HALF, HALF), HALF)
        for i, src in enumerate((mine_ref, got_ref)):
            at = 2 * s + i
            loads.append(pltpu.make_async_copy(src.at[:, cols], blocks.at[at], sems.at[at]))
    for load in loads:
        load.start()
    stores = []
    for s in range(NX):
        for i in range(2):
            loads[2 * s + i].wait()
            turned[s, :, i * HALF : (i + 1) * HALF] = blocks[2 * s + i].T
        stores.append(pltpu.make_async_copy(turned.at[s], out_ref.at[s], out_sems.at[s]))
        stores[s].start()
    for store in stores:
        store.wait()


def piece_of(w_ref, s, mine_ref, got_ref):
    out = jnp.dot(w_ref[s, :, :HALF], mine_ref[...], preferred_element_type=jnp.float32)
    return out + jnp.dot(w_ref[s, :, HALF:], got_ref[...], preferred_element_type=jnp.float32)


def piece_kernel(w_ref, mine_ref, got_ref, out_ref, *, s):
    out_ref[...] = piece_of(w_ref, s, mine_ref, got_ref).astype(jnp.bfloat16)


def mine_kernel(w_ref, mine_ref, got_ref, out_ref):
    out_ref[...] = piece_of(w_ref, 0, mine_ref, got_ref)


def sum_kernel(mine_ref, g1, g2, g3, out_ref):
    out = mine_ref[...]
    for g in (g1, g2, g3):
        out += g[...].astype(jnp.float32)
    out_ref[...] = out.astype(jnp.bfloat16)


def bf16(*shape):
    return jax.ShapeDtypeStruct(shape, jnp.bfloat16)


def f32(*shape):
    return jax.ShapeDtypeStruct(shape, jnp.float32)


def steps(queries, keys, values, block_ids, out_weight):
    z = lax.axis_index("z")
    y = lax.axis_index("y")
    x = lax.axis_index("x")
    core = lax.axis_index("core")
    vmem = pl.BlockSpec(memory_space=pltpu.VMEM)
    smem = pl.BlockSpec(memory_space=pltpu.SMEM)
    packed = pallas(
        60, pack_kernel, in_specs=[vmem] * 2, out_specs=vmem, out_shape=bf16(NY, SL, 2 * HD)
    )(keys, values)
    row = lax.all_to_all(packed, "y", 0, 0)
    ids = block_ids.reshape(HEADS * TOP)
    slot = jnp.zeros_like(ids)
    offset = (ids // NY - z) % NZ
    for d, place in enumerate(SLOTS):
        slot = jnp.where(offset == d, place, slot)
    code = jnp.where(ids < z * NY + y, slot * NY + ids % NY, NONE)
    kept = [row]
    p = m = row
    for k in range(1, HOPS + 1):
        p = lax.ppermute(p, "z", ahead(k))
        kept.append(p)
        if k < HOPS:
            m = lax.ppermute(m, "z", astern(k))
            kept.append(m)
    w_got = send(out_weight, "core", 1)
    qx = pallas(
        8, query_kernel, in_specs=[smem, vmem], out_specs=vmem, out_shape=bf16(EXT, TOK)
    )(code, queries)
    own, own_lse = pallas(
        8,
        own_kernel,
        in_specs=[vmem] * 3,
        out_specs=[vmem] * 2,
        out_shape=[bf16(HALF, TOK), f32(2 * HEADS, TOK)],
    )(qx, keys, values)
    order = (2, 1, 3)
    qs = [send(qx, "y", s) for s in order]
    codes = jnp.stack([a[HALF, : HEADS * TOP] for a in qs], axis=0).astype(jnp.int32).reshape(-1)
    cols = (x + jnp.arange(NX, dtype=jnp.int32)) % NX * 2 + core
    w = pallas(
        12,
        turn_kernel,
        in_specs=[smem] + [pl.BlockSpec(memory_space=pltpu.HBM)] * 2,
        out_specs=pl.BlockSpec(memory_space=pltpu.HBM),
        out_shape=bf16(NX, HALF, 2 * HALF),
        scratch_shapes=[
            pltpu.VMEM((2 * NX, HALF, HALF), jnp.bfloat16),
            pltpu.VMEM((NX, HALF, 2 * HALF), jnp.bfloat16),
            pltpu.SemaphoreType.DMA((2 * NX,)),
            pltpu.SemaphoreType.DMA((NX,)),
        ],
    )(cols, out_weight, w_got)
    kv = jnp.concatenate(kept, axis=0)

    def attend(code, *qs):
        return pallas(
            12,
            slices_kernel,
            in_specs=[smem] + [vmem] * (1 + len(qs)),
            out_specs=[vmem] * len(qs),
            out_shape=[bf16(EXT, TOK)] * len(qs),
        )(code, kv, *qs)

    parts = attend(codes, *qs)
    back = [send(part, "y", -s) for s, part in zip(order, parts)]
    (home,) = attend(code, qx)
    att = pallas(
        8, merge_kernel, in_specs=[vmem] * 6, out_specs=vmem, out_shape=bf16(HALF, TOK)
    )(own, own_lse, home, *back)
    att_got = send(att, "core", 1)
    got = []
    for s in order:
        part = pallas(
            12,
            functools.partial(piece_kernel, s=s),
            in_specs=[vmem] * 3,
            out_specs=vmem,
            out_shape=bf16(HALF, TOK),
        )(w, att, att_got)
        got.append(send(part, "x", s))
    mine = pallas(
        12, mine_kernel, in_specs=[vmem] * 3, out_specs=vmem, out_shape=f32(HALF, TOK)
    )(w, att, att_got)
    return pallas(
        8, sum_kernel, in_specs=[vmem] * 4, out_specs=vmem, out_shape=bf16(HALF, TOK)
    )(mine, *got)


def solution(mesh):
    axes = ("z", "y", "x", "core")
    grid = Mesh(mesh.devices.reshape(NZ, NY, NX, 2), axes)
    rows, cols = axes[:2], axes[2:]
    return jax.shard_map(
        steps,
        mesh=grid,
        in_specs=(P(rows, cols), P(rows, cols), P(rows, cols), P(rows, cols, None), P(cols, None)),
        out_specs=P(cols, rows),
        check_vma=False,
    )
```

```python
import functools
import math

import jax
import jax.numpy as jnp
from jax import lax
from jax.experimental import pallas as pl
from jax.experimental.pallas import tpu as pltpu
from jax.sharding import Mesh, PartitionSpec as P


HD = 128
HEADS = 4
HALF = HEADS * HD
TOP = 3
NZ, NY, NX = 16, 4, 4
TOK = 384
SL = TOK // NY
EXT = HALF + 16
LOG2E = 1.4426950408889634
COEF = LOG2E / math.sqrt(HD)
DEAD = -1e30
NONE = NZ * NY
HOPS = NZ // 2
SLOTS = tuple(2 * d if d < HOPS else 2 * (NZ - d) - 1 for d in range(NZ))


def pallas(mib, kernel, **kw):
    grant = pltpu.CompilerParams(vmem_limit_bytes=mib * 1024 * 1024)
    return pl.pallas_call(kernel, compiler_params=grant, **kw)


def send(a, axis, s):
    n = lax.axis_size(axis)
    return lax.ppermute(a, axis, [(i, (i + s) % n) for i in range(n)])


def ahead(k):
    return [(i, i + 1) for i in range(k - 1, NZ - 1)]


def astern(k):
    return [((r - k + 1) % NZ, (r - k) % NZ) for r in range(HOPS - 1)]


def tn(a, b):
    return lax.dot_general(a, b, (((0,), (0,)), ((), ())), preferred_element_type=jnp.float32)


def pack_kernel(k_ref, v_ref, out_ref):
    for y in range(NY):
        out_ref[y, :, :HD] = k_ref[y * SL : (y + 1) * SL, :]
        out_ref[y, :, HD:] = v_ref[y * SL : (y + 1) * SL, :]


def query_kernel(code_ref, q_ref, qx_ref):
    for h in range(HEADS):
        qx_ref[h * HD : (h + 1) * HD, :] = q_ref[:, h * HD : (h + 1) * HD].T
    lane = lax.broadcasted_iota(jnp.int32, (16, TOK), 1)
    codes = jnp.zeros((16, TOK), jnp.float32)
    for i in range(HEADS * TOP):
        codes = jnp.where(lane == i, code_ref[i].astype(jnp.float32), codes)
    qx_ref[HALF:, :] = codes.astype(jnp.bfloat16)


def own_kernel(q_ref, k_ref, v_ref, o_ref, lse_ref):
    keep = lax.broadcasted_iota(jnp.int32, (TOK, TOK), 0) <= lax.broadcasted_iota(
        jnp.int32, (TOK, TOK), 1
    )
    k = k_ref[...]
    v = v_ref[...]
    rows = []
    for h in range(HEADS):
        q = q_ref[h * HD : (h + 1) * HD, :]
        s = jnp.dot(k, q, preferred_element_type=jnp.float32)
        s = jnp.where(keep, s * COEF, DEAD)
        top = jnp.max(s, axis=0, keepdims=True)
        p = jnp.exp2(s - top)
        total = jnp.sum(p, axis=0, keepdims=True)
        o = tn(v, p.astype(jnp.bfloat16)) * (1.0 / total)
        o_ref[h * HD : (h + 1) * HD, :] = o.astype(jnp.bfloat16)
        rows.append(top + jnp.log2(total))
    lse_ref[...] = jnp.concatenate(rows + rows, axis=0)


def slices_of(code_ref, kv_ref, q_ref, o_ref, base):
    rows = []
    for h in range(HEADS):
        codes = [code_ref[base + h * TOP + j] for j in range(TOP)]
        picked = [kv_ref[jnp.minimum(c, NONE - 1)] for c in codes]
        bias = [jnp.where(c < NONE, 0.0, DEAD).astype(jnp.float32) for c in codes]
        k = jnp.concatenate([t[:, :HD] for t in picked], axis=0)
        v = jnp.concatenate([t[:, HD:] for t in picked], axis=0)
        s = jnp.dot(k, q_ref[h * HD : (h + 1) * HD, :], preferred_element_type=jnp.float32)
        s = [s[j * SL : (j + 1) * SL] * COEF + bias[j] for j in range(TOP)]
        s = jnp.concatenate(s, axis=0)
        top = jnp.max(s, axis=0, keepdims=True)
        p = jnp.exp2(s - top)
        total = jnp.sum(p, axis=0, keepdims=True)
        o = tn(v, p.astype(jnp.bfloat16)) * (1.0 / total)
        o_ref[h * HD : (h + 1) * HD, :] = o.astype(jnp.bfloat16)
        lse = top + jnp.log2(total)
        hi = lse.astype(jnp.bfloat16).astype(jnp.float32)
        mid = (lse - hi).astype(jnp.bfloat16).astype(jnp.float32)
        rows += [hi, mid, lse - hi - mid]
    rows += [jnp.zeros((4, TOK), jnp.float32)]
    o_ref[HALF:, :] = jnp.concatenate(rows, axis=0).astype(jnp.bfloat16)


def slices_kernel(code_ref, kv_ref, *rest):
    n = len(rest) // 2
    for i in range(n):
        slices_of(code_ref, kv_ref, rest[i], rest[n + i], i * HEADS * TOP)


def merge_kernel(own_ref, lse_ref, p0, p1, p2, p3, out_ref):
    parts = (p0, p1, p2, p3)
    tails = [p[HALF:, :].astype(jnp.float32) for p in parts]
    for h in range(HEADS):
        span = slice(h * HD, (h + 1) * HD)
        own = lse_ref[h : h + 1, :]
        lses = [
            t[3 * h : 3 * h + 1] + t[3 * h + 1 : 3 * h + 2] + t[3 * h + 2 : 3 * h + 3]
            for t in tails
        ]
        top = own
        for x in lses:
            top = jnp.maximum(top, x)
        w = jnp.exp2(own - top)
        total = w
        acc = w * own_ref[span, :].astype(jnp.float32)
        for p, x in zip(parts, lses):
            w = jnp.exp2(x - top)
            total = total + w
            acc = acc + w * p[span, :].astype(jnp.float32)
        out_ref[span, :] = (acc * (1.0 / total)).astype(jnp.bfloat16)


def turn_kernel(cols_ref, src_ref, out_ref, blocks, turned, sems, out_sems):
    loads = []
    for s in range(NX):
        cols = pl.ds(pl.multiple_of(cols_ref[s] * HALF, HALF), HALF)
        loads.append(pltpu.make_async_copy(src_ref.at[:, cols], blocks.at[s], sems.at[s]))
    for load in loads:
        load.start()
    stores = []
    for s in range(NX):
        loads[s].wait()
        turned[s] = blocks[s].T
        stores.append(pltpu.make_async_copy(turned.at[s], out_ref.at[s], out_sems.at[s]))
        stores[s].start()
    for store in stores:
        store.wait()


def piece_of(w_mine, w_got, s, mine_ref, got_ref):
    out = jnp.dot(w_mine[s], mine_ref[...], preferred_element_type=jnp.float32)
    return out + jnp.dot(w_got[s], got_ref[...], preferred_element_type=jnp.float32)


def piece_kernel(w_mine, w_got, mine_ref, got_ref, out_ref, *, s):
    out_ref[...] = piece_of(w_mine, w_got, s, mine_ref, got_ref).astype(jnp.bfloat16)


def mine_kernel(w_mine, w_got, mine_ref, got_ref, out_ref):
    out_ref[...] = piece_of(w_mine, w_got, 0, mine_ref, got_ref)


def sum_kernel(mine_ref, g1, g2, g3, out_ref):
    out = mine_ref[...]
    for g in (g1, g2, g3):
        out += g[...].astype(jnp.float32)
    out_ref[...] = out.astype(jnp.bfloat16)


def bf16(*shape):
    return jax.ShapeDtypeStruct(shape, jnp.bfloat16)


def f32(*shape):
    return jax.ShapeDtypeStruct(shape, jnp.float32)


def steps(queries, keys, values, block_ids, out_weight):
    z = lax.axis_index("z")
    y = lax.axis_index("y")
    x = lax.axis_index("x")
    core = lax.axis_index("core")
    vmem = pl.BlockSpec(memory_space=pltpu.VMEM)
    smem = pl.BlockSpec(memory_space=pltpu.SMEM)
    packed = pallas(
        60, pack_kernel, in_specs=[vmem] * 2, out_specs=vmem, out_shape=bf16(NY, SL, 2 * HD)
    )(keys, values)
    row = lax.all_to_all(packed, "y", 0, 0)
    ids = block_ids.reshape(HEADS * TOP)
    slot = jnp.zeros_like(ids)
    offset = (ids // NY - z) % NZ
    for d, place in enumerate(SLOTS):
        slot = jnp.where(offset == d, place, slot)
    code = jnp.where(ids < z * NY + y, slot * NY + ids % NY, NONE)
    kept = [row]
    p = m = row
    for k in range(1, HOPS + 1):
        p = lax.ppermute(p, "z", ahead(k))
        kept.append(p)
        if k < HOPS:
            m = lax.ppermute(m, "z", astern(k))
            kept.append(m)
    w_got = send(out_weight, "core", 1)
    qx = pallas(
        8, query_kernel, in_specs=[smem, vmem], out_specs=vmem, out_shape=bf16(EXT, TOK)
    )(code, queries)
    own, own_lse = pallas(
        8,
        own_kernel,
        in_specs=[vmem] * 3,
        out_specs=[vmem] * 2,
        out_shape=[bf16(HALF, TOK), f32(2 * HEADS, TOK)],
    )(qx, keys, values)
    order = (2, 1, 3)
    qs = [send(qx, "y", s) for s in order]
    codes = jnp.stack([a[HALF, : HEADS * TOP] for a in qs], axis=0).astype(jnp.int32).reshape(-1)
    cols = (x + jnp.arange(NX, dtype=jnp.int32)) % NX * 2 + core
    hbm = pl.BlockSpec(memory_space=pltpu.HBM)

    def turn(src):
        return pallas(
            8,
            turn_kernel,
            in_specs=[smem, hbm],
            out_specs=hbm,
            out_shape=bf16(NX, HALF, HALF),
            scratch_shapes=[
                pltpu.VMEM((NX, HALF, HALF), jnp.bfloat16),
                pltpu.VMEM((NX, HALF, HALF), jnp.bfloat16),
                pltpu.SemaphoreType.DMA((NX,)),
                pltpu.SemaphoreType.DMA((NX,)),
            ],
        )(cols, src)

    wt = (turn(out_weight), turn(w_got))
    kv = jnp.concatenate(kept, axis=0)

    def attend(code, *qs):
        return pallas(
            12,
            slices_kernel,
            in_specs=[smem] + [vmem] * (1 + len(qs)),
            out_specs=[vmem] * len(qs),
            out_shape=[bf16(EXT, TOK)] * len(qs),
        )(code, kv, *qs)

    parts = attend(codes, *qs)
    back = [send(part, "y", -s) for s, part in zip(order, parts)]
    (home,) = attend(code, qx)
    att = pallas(
        8, merge_kernel, in_specs=[vmem] * 6, out_specs=vmem, out_shape=bf16(HALF, TOK)
    )(own, own_lse, home, *back)
    att_got = send(att, "core", 1)
    got = []
    for s in order:
        part = pallas(
            12,
            functools.partial(piece_kernel, s=s),
            in_specs=[vmem] * 4,
            out_specs=vmem,
            out_shape=bf16(HALF, TOK),
        )(*wt, att, att_got)
        got.append(send(part, "x", s))
    mine = pallas(
        12, mine_kernel, in_specs=[vmem] * 4, out_specs=vmem, out_shape=f32(HALF, TOK)
    )(*wt, att, att_got)
    return pallas(
        8, sum_kernel, in_specs=[vmem] * 4, out_specs=vmem, out_shape=bf16(HALF, TOK)
    )(mine, *got)


def solution(mesh):
    axes = ("z", "y", "x", "core")
    grid = Mesh(mesh.devices.reshape(NZ, NY, NX, 2), axes)
    rows, cols = axes[:2], axes[2:]
    return jax.shard_map(
        steps,
        mesh=grid,
        in_specs=(P(rows, cols), P(rows, cols), P(rows, cols), P(rows, cols, None), P(cols, None)),
        out_specs=P(cols, rows),
        check_vma=False,
    )
```
